32 devices in a mesh: tm: 4 (over y, x), sat: 8 (over z, core).
Axes of the slice: x: 2, y: 2, z: 4, core: 2. Of those that a mesh axis runs over, the one named last changes fastest.
Arguments:
- samples: int32 [2, 8, 8192], P(None, 'tm', 'sat'), may hold values from -1073741824 to 1073741823
- codes: int32 [24, 4092], P('sat'), may hold values from -1 to 1, as said below
- dopplers: int32 [16], replicated, may hold values from -60 to 60
Outputs:
- power: float32 [16, 24, 8192], P('tm', 'sat')
- detection: float32 [24], P('sat')
The draws below stay inside these ranges and needn't reach their ends.
Inputs may be any that keep to these rules, and one draw needn't show every extreme that they name: `codes`: each entry is -1 or 1.
All inputs are finite; a program needn't handle non-finite values.
Results may differ from the reference program's by a relative error of at most 0.0003.
Values sent between devices are 32-bit elements.
A program may use at most 64 MiB of HBM per device.

```python
import math
import jax
import jax.numpy as jnp
from jax import lax

N = 8192
CHIPS = 4092
BLOCK_COUNT = 8
DOPPLER = 16
SATS = 24


def draw_samples(key, part):
    key_raw = jax.random.fold_in(key, 11)
    key_shift = jax.random.fold_in(key, 12)
    raw_words = jax.random.randint(key_raw, (2, BLOCK_COUNT, N), -1073741824, 1073741824, dtype=jnp.int32)
    shifts = jax.random.randint(key_shift, (2, BLOCK_COUNT, 32), 0, 3, dtype=jnp.int32)
    shifts = jnp.repeat(shifts, N // 32, axis=2)
    return jnp.right_shift(raw_words, shifts)


def draw_codes(key, part):
    chip_bits = jax.random.randint(jax.random.fold_in(key, 21), (SATS, CHIPS), 0, 2, dtype=jnp.int32)
    return 2 * chip_bits - 1


def with_ends(entries, stream_key, smallest, top_value):
    spot = [jax.random.randint(jax.random.fold_in(stream_key, axis), (), 0, length) for axis, length in enumerate(entries.shape)]
    main_axis = entries.shape.index(max(entries.shape))
    neighbour = spot[:main_axis] + [(spot[main_axis] + 1) % entries.shape[main_axis]] + spot[main_axis + 1:]
    return entries.at[tuple(spot)].set(smallest).at[tuple(neighbour)].set(top_value)


def setup_inputs(seed: int = 0) -> dict:
    seeds = jax.random.split(jax.random.key(seed), 4)
    return {
        "samples": draw_samples(jax.random.fold_in(seeds[3], 71), 0),
        "codes": draw_codes(jax.random.fold_in(seeds[3], 71), 0),
        "dopplers": with_ends(jax.random.randint(seeds[2], (DOPPLER,), -60, 61), jax.random.fold_in(seeds[2], 1), -60, 60).astype(jnp.int32),
    }


sample_scale = 2.0 ** -29
wrap_count = 32768


def replica_rows(codes):
    offsets = jnp.arange(N, dtype=jnp.int32)
    chip_index = (offsets * CHIPS) // N
    halves = jnp.mod((offsets * (2 * CHIPS)) // N, 2)
    sign_rows = (1 - 2 * halves).astype(jnp.float32)
    return jnp.take(codes, chip_index, axis=1).astype(jnp.float32) * sign_rows[None, :]


def reference(samples, codes, dopplers):
    real_part = samples[0].astype(jnp.float32) * sample_scale
    imag_part = samples[1].astype(jnp.float32) * sample_scale
    received_record = lax.complex(real_part, imag_part)
    spectrum = jnp.conj(jnp.fft.fft(replica_rows(codes), axis=-1))
    offsets = jnp.arange(N, dtype=jnp.int32)

    def one_bin(doppler_bin):
        rotation_angles = jnp.mod(doppler_bin * offsets, wrap_count).astype(jnp.float32) * (2.0 * math.pi / wrap_count)
        doppler_mixer = lax.complex(jnp.cos(rotation_angles), -jnp.sin(rotation_angles))
        wiped_record = jnp.fft.fft(received_record * doppler_mixer[None, :], axis=-1)

        def one_sat(code_spec):
            lagged = jnp.fft.ifft(wiped_record * code_spec[None, :], axis=-1)
            return jnp.sum(jnp.real(lagged) ** 2 + jnp.imag(lagged) ** 2, axis=0)

        return lax.map(one_sat, spectrum)

    power_map = lax.map(one_bin, dopplers) * (1.0 / (N * BLOCK_COUNT))
    average_energy = jnp.sum(real_part * real_part + imag_part * imag_part) / (BLOCK_COUNT * N)
    peak_value = jnp.max(power_map, axis=(0, 2))
    detection = peak_value / jnp.maximum(average_energy, 0.25)
    return (power_map, detection)
```

```python
import functools
import math

import jax
import jax.numpy as jnp
import ml_dtypes
import numpy as np
from jax import lax
from jax.experimental import pallas as pl
from jax.experimental.pallas import tpu as pltpu
from jax.sharding import PartitionSpec as P

sample_scale = 2.0 ** (-29)
wrap_count = 32768
LANES = 128
KERNEL_BYTES = 55_800_000
PADDING = 1_200_000
MESH = pl.DeviceIdType.MESH


def halves(table):
    high = table.astype(np.float32).astype(ml_dtypes.bfloat16)
    low = (table - high.astype(np.float64)).astype(np.float32).astype(ml_dtypes.bfloat16)
    return high, low


@functools.lru_cache(maxsize=None)
def tables(sample_length, chip_count):
    inner = LANES
    outer = sample_length // inner
    a = np.arange(outer)
    c = np.arange(inner)
    ang_o = 2 * np.pi * (np.outer(a, a) % outer) / outer
    ang_t = 2 * np.pi * (np.outer(a, c) % sample_length) / sample_length
    ang_i = 2 * np.pi * (np.outer(c, c) % inner) / inner
    fc, fs = np.cos(ang_o), -np.sin(ang_o)
    first = np.block([[fc, -fs], [fs, fc]])
    second = np.block([[-fs, -fc], [fc, -fs]])
    wc, ws = np.cos(ang_i), -np.sin(ang_i)
    fh, fl = halves(np.block([[wc, ws], [-ws, wc]]))
    ih, il = halves(np.block([[wc, -ws], [ws, wc]]))
    bh, bl = halves(np.block([[fc, fs], [-fs, fc]]))
    ch, cl = halves(np.concatenate([fc, fs], axis=0))
    offsets = np.arange(sample_length).reshape(outer, inner)
    chips = offsets * chip_count // sample_length
    signs = 1 - 2 * ((offsets * 2 * chip_count // sample_length) % 2)
    starts = tuple(int(v) for v in chips[:, 0])
    within = chips - chips[:, :1]
    wide = np.concatenate([fh, fh, fl, ih, ih, il], axis=0)
    narrow = [first, second, np.cos(ang_t), -np.sin(ang_t), bh, bl,
              np.concatenate([ch, cl], axis=1), within, signs]
    narrow = np.concatenate([np.asarray(t, np.float32) for t in narrow], axis=0)
    return wide, narrow, starts


def padded(table, size):
    extra = -(-size // (table.shape[1] * table.dtype.itemsize)) - table.shape[0]
    return np.pad(table, ((0, max(extra, 0)), (0, 0)))


def split(value):
    high = value.astype(jnp.bfloat16)
    low = (value - high.astype(jnp.float32)).astype(jnp.bfloat16)
    return high, low


def mm(left, right):
    return jnp.dot(left, right, preferred_element_type=jnp.float32)


def flip(me, k, count):
    if count & (count - 1):
        return lax.rem(me + k, count)
    peer, bit = 0, 1
    while bit < count:
        peer = peer + ((me // bit + k // bit) % 2) * bit
        bit *= 2
    return peer


def back_flip(me, k, count):
    return lax.rem(me + count - k, count) if count & (count - 1) else flip(me, k, count)


def kernel(starts, outer, chip_count, cores, x_hbm, codes_hbm, dop_hbm, wide_hbm, narrow_hbm,
           power_ref, peak_ref, chips, dop_ref, wide, narrow, back,
           everyone, cpad, gath, cspec, rot, dtw, xs, spec, lagged, acc, peaks, mine,
           tab_sem, send_z, recv_z, send_tm, recv_tm, send_peak, recv_peak):
    inner = LANES
    tm_count, _, line, _, packed_rows, _ = everyone.shape
    dop_rows, sats = acc.shape[0], acc.shape[1]
    sample_length = outer * inner
    rows = outer // (cores * line)
    own = packed_rows // rows
    blocks = tm_count * own
    slots = spec.shape[0]
    me_tm, me_sat = lax.axis_index("tm"), lax.axis_index("sat")
    me_z, me_core = me_sat // cores, lax.rem(me_sat, cores)

    def place(z, core):
        return z * cores + core

    near = [(k, c) for k in range(line) for c in range(cores) if k or c]
    barrier = pltpu.get_barrier_semaphore()
    for k, c in near:
        target = place(flip(me_z, k, line), flip(me_core, c, cores))
        pl.semaphore_signal(barrier, inc=1, device_id={"sat": target}, device_id_type=MESH)
    for k in range(1, tm_count):
        for c in range(cores):
            target = place(me_z, flip(me_core, c, cores))
            pl.semaphore_signal(
                barrier, inc=1, device_id={"tm": flip(me_tm, k, tm_count), "sat": target}, device_id_type=MESH)

    pairs = ((x_hbm, everyone.at[me_tm, me_core, me_z]), (codes_hbm, chips), (dop_hbm, dop_ref),
             (narrow_hbm.at[pl.ds(0, narrow.shape[0])], narrow),
             (wide_hbm.at[pl.ds(0, wide.shape[0])], wide))
    loads = [pltpu.make_async_copy(h, t, tab_sem.at[i]) for i, (h, t) in enumerate(pairs)]
    for load in loads:
        load.start()

    def along_z(k, c):
        here = everyone.at[me_tm, me_core, me_z]
        target = place(flip(me_z, k, line), flip(me_core, c, cores))
        return pltpu.make_async_remote_copy(
            src_ref=here, dst_ref=here, send_sem=send_z.at[k * cores + c], recv_sem=recv_z.at[k * cores + c],
            device_id={"sat": target}, device_id_type=MESH)

    def from_z(k, c):
        there = everyone.at[me_tm, back_flip(me_core, c, cores), back_flip(me_z, k, line)]
        return pltpu.make_async_remote_copy(
            src_ref=there, dst_ref=there, send_sem=send_z.at[k * cores + c], recv_sem=recv_z.at[k * cores + c],
            device_id={"sat": me_sat}, device_id_type=MESH)

    def relay(k, z):
        for c in range(cores):
            piece = everyone.at[me_tm, me_core, z]
            pltpu.make_async_remote_copy(
                src_ref=piece, dst_ref=piece, send_sem=send_tm.at[k - 1], recv_sem=recv_tm.at[k - 1],
                device_id={"tm": flip(me_tm, k, tm_count), "sat": place(me_z, flip(me_core, c, cores))},
                device_id_type=MESH).start()

    def whole_group(k, at):
        return pltpu.make_async_remote_copy(
            src_ref=everyone.at[at], dst_ref=everyone.at[at], send_sem=send_tm.at[k - 1],
            recv_sem=recv_tm.at[k - 1], device_id={"tm": flip(me_tm, k, tm_count)}, device_id_type=MESH)

    def share_peak(k):
        return pltpu.make_async_remote_copy(
            src_ref=mine, dst_ref=peaks.at[k - 1], send_sem=send_peak.at[k - 1],
            recv_sem=recv_peak.at[k - 1], device_id={"tm": flip(me_tm, k, tm_count)}, device_id_type=MESH)

    early = range(1, max(tm_count - 1, 2)) if tm_count > 1 else ()
    late = [k for k in range(1, tm_count) if k not in early]

    loads[0].wait()
    pl.semaphore_wait(barrier, len(near) + (tm_count - 1) * cores)
    for k, c in reversed(near):
        along_z(k, c).start()
    for k in early:
        relay(k, me_z)

    loads[1].wait()
    cpad[...] = jnp.zeros_like(cpad)
    cpad[0:sats, 0:chip_count] = chips[...].astype(jnp.float32)
    for n1 in range(outer):
        base = starts[n1] // LANES * LANES
        shift = starts[n1] - base
        piece = cpad[:, base:base + 2 * LANES]
        if shift:
            piece = pltpu.roll(piece, 2 * LANES - shift, 1)
        for s in range(sats):
            gath[s, n1:n1 + 1, :] = piece[s:s + 1, :LANES]
    for load in loads[2:]:
        load.wait()

    cut = [0]

    def take(count):
        cut.append(cut[-1] + count)
        return narrow[cut[-2]:cut[-1]]

    first, second = take(2 * outer), take(2 * outer)
    t_re, t_im = take(outer), take(outer)
    bh, bl = take(2 * outer).astype(jnp.bfloat16), take(2 * outer).astype(jnp.bfloat16)
    back[...] = jnp.concatenate([bh, bh, bl], axis=1)
    code = take(2 * outer).astype(jnp.bfloat16)
    within = take(outer).astype(jnp.int32)
    signs = take(outer)
    t_at = 4 * outer
    fwd_ref = wide.at[pl.ds(0, 6 * inner)]
    inv_ref = wide.at[pl.ds(6 * inner, 6 * inner)]
    scale = math.sqrt(1.0 / (float(sample_length) ** 3 * blocks))
    for s in range(sats):
        rep = jnp.take_along_axis(gath[s], within, axis=1) * signs
        rep = rep.astype(jnp.bfloat16)
        y = mm(code, jnp.concatenate([rep, rep], axis=0))
        y_re, y_im = y[:outer], y[outer:]
        z = jnp.concatenate([y_re * t_re - y_im * t_im, y_re * t_im + y_im * t_re], axis=1)
        zh, zl = split(z)
        cspec[s] = mm(jnp.concatenate([zh, zl, zh], axis=1), fwd_ref[...]) * scale

    lane = lax.broadcasted_iota(jnp.int32, (8, inner), 1)
    row_of = lax.rem(lane, outer) * inner
    base_row = me_tm * dop_rows
    turn = 2.0 * math.pi / wrap_count
    bins = lax.broadcasted_iota(jnp.int32, (8, inner), 0)
    for f0 in range(0, dop_rows, 4):
        d = jnp.zeros((8, inner), jnp.int32)
        for f in range(f0, min(f0 + 4, dop_rows)):
            d = jnp.where(lax.rem(bins, 4) == f - f0, dop_ref[base_row + f], d)
        m = (jnp.where(bins < 4, row_of, lane) * d) & (wrap_count - 1)
        angle = m.astype(jnp.float32) * turn
        cosine, sine = jnp.cos(angle), -jnp.sin(angle)
        for f in range(f0, min(f0 + 4, dop_rows)):
            i = f - f0
            c1, s1 = cosine[i:i + 1] * sample_scale, sine[i:i + 1] * sample_scale
            c2, s2 = cosine[i + 4:i + 5], sine[i + 4:i + 5]
            mh, ml = split(first * c1 + second * s1)
            rot[f] = jnp.concatenate([mh, mh, ml], axis=1)
            dtw[f, 0] = t_re * c2 - t_im * s2
            dtw[f, 1] = t_re * s2 + t_im * c2
    acc[...] = jnp.zeros_like(acc)

    for k in range(1, line):
        from_z(k, 0).wait_recv()
        for j in early:
            relay(j, back_flip(me_z, k, line))
    for j in late:
        for k in range(line):
            relay(j, back_flip(me_z, k, line))
    for k, c in near:
        if c:
            from_z(k, c).wait_recv()

    def arrive(j):
        g = back_flip(me_tm, j, tm_count)
        for blk in range(own):
            parts = [everyone[g, q % cores, q // cores, part, pl.ds(blk, rows, stride=own), :]
                     for part in range(2) for q in range(cores * line)]
            x = jnp.concatenate(parts, axis=0).astype(jnp.float32)
            xh, xl = split(x)
            at = slice(blk * inner, (blk + 1) * inner)
            xs[0:2 * outer, at] = xh
            xs[2 * outer:4 * outer, at] = xl
            xs[4 * outer:6 * outer, at] = xh

    def rotate(f):
        return mm(rot[f], xs[...])

    def spectrum(f, y):
        u_re, u_im = dtw[f, 0], dtw[f, 1]
        zs = []
        for blk in range(own):
            y_re = y[:outer, blk * inner:(blk + 1) * inner]
            y_im = y[outer:, blk * inner:(blk + 1) * inner]
            zs.append(jnp.concatenate([y_re * u_re - y_im * u_im, y_re * u_im + y_im * u_re], axis=1))
        zh, zl = split(jnp.concatenate(zs, axis=0))
        spec[f % slots] = mm(jnp.concatenate([zh, zl, zh], axis=1), fwd_ref[...])

    def cross(f):
        crosses = []
        for s in range(sats):
            k_re, k_im = cspec[s, :, :inner], cspec[s, :, inner:]
            for blk in range(own):
                s_re = spec[f % slots, blk * outer:(blk + 1) * outer, :inner]
                s_im = spec[f % slots, blk * outer:(blk + 1) * outer, inner:]
                crosses.append(jnp.concatenate(
                    [s_re * k_re + s_im * k_im, s_im * k_re - s_re * k_im], axis=1))
        ch, cl = split(jnp.concatenate(crosses, axis=0))
        lag = mm(jnp.concatenate([ch, cl, ch], axis=1), inv_ref[...])
        w_re, w_im = narrow[t_at:t_at + outer], narrow[t_at + outer:t_at + 2 * outer]
        for s in range(sats):
            for blk in range(own):
                at = (s * own + blk) * outer
                l_re, l_im = lag[at:at + outer, :inner], lag[at:at + outer, inner:]
                wh, wl = split(jnp.concatenate(
                    [l_re * w_re + l_im * w_im, l_im * w_re - l_re * w_im], axis=0))
                to = slice(blk * inner, (blk + 1) * inner)
                lagged[f % slots, s, 0:2 * outer, to] = wh
                lagged[f % slots, s, 2 * outer:4 * outer, to] = wl

    def finish(f):
        for s in range(sats):
            high, low = lagged[f % slots, s, 0:2 * outer], lagged[f % slots, s, 2 * outer:4 * outer]
            out = mm(back[...], jnp.concatenate([high, low, high], axis=0))
            o_re, o_im = out[:outer], out[outer:]
            p = o_re * o_re + o_im * o_im
            total = p[:, :inner]
            for blk in range(1, own):
                total = total + p[:, blk * inner:(blk + 1) * inner]
            acc[f, s] += total

    def item(index):
        return index // dop_rows, index % dop_rows

    def step(at, c_index, b_index, a_index, total):
        if a_index is not None and 0 <= a_index < total:
            j, f = item(a_index)
            if f == 0:
                if a_index:
                    whole_group(at + j, back_flip(me_tm, at + j, tm_count)).wait_recv()
                arrive(at + j)
        if 0 <= c_index < total:
            finish(item(c_index)[1])
        if 0 <= a_index < total:
            y = rotate(item(a_index)[1])
        if 0 <= b_index < total:
            cross(item(b_index)[1])
        if 0 <= a_index < total:
            spectrum(item(a_index)[1], y)

    total = tm_count * dop_rows
    for t in range(-3, total):
        step(0, t, t + 2, t + 3, total)

    mine[...] = jnp.zeros_like(mine)
    for s in range(sats):
        top = acc[0, s]
        for f in range(1, dop_rows):
            top = jnp.maximum(top, acc[f, s])
        mine[s:s + 1, :] = jnp.max(top, axis=0, keepdims=True)
    for k in range(1, tm_count):
        share_peak(k).start()
    for f in range(dop_rows):
        for s in range(sats):
            power_ref[s, :, f, :] = acc[f, s]
    energy = jnp.zeros((8, inner), jnp.float32)
    for g in range(tm_count):
        x = everyone[g].astype(jnp.float32)
        energy = energy + jnp.sum((x * x).reshape(-1, 8, inner), axis=0)
    mean = jnp.sum(energy) * (sample_scale * sample_scale / float(blocks * sample_length))
    floor = jnp.maximum(mean, 0.25)
    for k, c in near:
        along_z(k, c).wait_send()
    for k in range(1, tm_count):
        whole_group(k, me_tm).wait_send()
    for k in range(1, tm_count):
        share_peak(k).wait()
    best = mine[...]
    for k in range(1, tm_count):
        best = jnp.maximum(best, peaks[k - 1])
    best = jnp.max(best, axis=1, keepdims=True)
    peak_ref[...] = jnp.broadcast_to(best / floor, peak_ref.shape)


def shards(samples, codes, dopplers):
    tm_count, sat_count = lax.axis_size("tm"), lax.axis_size("sat")
    own, segment = samples.shape[1], samples.shape[2]
    sample_length = segment * sat_count
    outer, rows = sample_length // LANES, segment // LANES
    sats, chip_count = codes.shape
    dop_rows = dopplers.shape[0] // tm_count
    cores = 2 if sat_count % 2 == 0 else 1
    line = sat_count // cores
    wide, narrow, starts = tables(sample_length, chip_count)
    pad = (max(starts) // LANES + 2) * LANES
    pad = max(pad, -(-chip_count // LANES) * LANES)
    peak_rows = -(-sats // 8) * 8
    slots = dop_rows if dop_rows % 2 else 2
    vm = pl.BlockSpec(memory_space=pltpu.VMEM)
    hbm = pl.BlockSpec(memory_space=pltpu.HBM)
    dma = pltpu.SemaphoreType.DMA
    packed = samples.reshape(2, own, rows, LANES).transpose(0, 2, 1, 3).reshape(2, rows * own, LANES)
    power, peak = pl.pallas_call(
        functools.partial(kernel, starts, outer, chip_count, cores),
        out_shape=(
            jax.ShapeDtypeStruct((sats, outer, dop_rows, LANES), jnp.float32),
            jax.ShapeDtypeStruct((peak_rows, LANES), jnp.float32),
        ),
        in_specs=[hbm, hbm, hbm, hbm, hbm],
        out_specs=(vm, vm),
        scratch_shapes=[
            pltpu.VMEM(codes.shape, jnp.int32),
            pltpu.SMEM(dopplers.shape, jnp.int32),
            pltpu.VMEM(wide.shape, jnp.bfloat16),
            pltpu.VMEM(narrow.shape, jnp.float32),
            pltpu.VMEM((2 * outer, 6 * outer), jnp.bfloat16),
            pltpu.VMEM((tm_count, cores, line, 2, rows * own, LANES), jnp.int32),
            pltpu.VMEM((8, pad), jnp.float32),
            pltpu.VMEM((sats, outer, LANES), jnp.float32),
            pltpu.VMEM((sats, outer, 2 * LANES), jnp.float32),
            pltpu.VMEM((dop_rows, 2 * outer, 6 * outer), jnp.bfloat16),
            pltpu.VMEM((dop_rows, 2, outer, LANES), jnp.float32),
            pltpu.VMEM((6 * outer, own * LANES), jnp.bfloat16),
            pltpu.VMEM((slots, own * outer, 2 * LANES), jnp.float32),
            pltpu.VMEM((slots, sats, 4 * outer, own * LANES), jnp.bfloat16),
            pltpu.VMEM((dop_rows, sats, outer, LANES), jnp.float32),
            pltpu.VMEM((tm_count - 1, peak_rows, LANES), jnp.float32),
            pltpu.VMEM((peak_rows, LANES), jnp.float32),
            dma((5,)),
            dma((sat_count,)),
            dma((sat_count,)),
            dma((tm_count - 1,)),
            dma((tm_count - 1,)),
            dma((tm_count - 1,)),
            dma((tm_count - 1,)),
        ],
        compiler_params=pltpu.CompilerParams(
            vmem_limit_bytes=KERNEL_BYTES, collective_id=0, has_side_effects=True),
        name="search",
    )(packed, codes, dopplers, jnp.asarray(padded(wide, PADDING)), jnp.asarray(padded(narrow, PADDING)))
    power = power.transpose(2, 0, 1, 3).reshape(dop_rows, sats, sample_length)
    return power, peak[:sats, 0]


def solution(mesh):
    placed = (P(None, "tm", "sat"), P("sat", None), P())
    return jax.shard_map(
        shards,
        mesh=mesh,
        in_specs=placed,
        out_specs=(P("tm", "sat", None), P("sat")),
        check_vma=False,
    )
```

```python
import functools
import math

import jax
import jax.numpy as jnp
import ml_dtypes
import numpy as np
from jax import lax
from jax.experimental import pallas as pl
from jax.experimental.pallas import tpu as pltpu
from jax.sharding import PartitionSpec as P

sample_scale = 2.0 ** (-29)
wrap_count = 32768
LANES = 128
KERNEL_BYTES = 55_800_000
PADDING = 1_200_000
MESH = pl.DeviceIdType.MESH


def halves(table):
    high = table.astype(np.float32).astype(ml_dtypes.bfloat16)
    low = (table - high.astype(np.float64)).astype(np.float32).astype(ml_dtypes.bfloat16)
    return high, low


@functools.lru_cache(maxsize=None)
def tables(sample_length, chip_count):
    inner = LANES
    outer = sample_length // inner
    a = np.arange(outer)
    c = np.arange(inner)
    ang_o = 2 * np.pi * (np.outer(a, a) % outer) / outer
    ang_t = 2 * np.pi * (np.outer(a, c) % sample_length) / sample_length
    ang_i = 2 * np.pi * (np.outer(c, c) % inner) / inner
    fc, fs = np.cos(ang_o), -np.sin(ang_o)
    first = np.block([[fc, -fs], [fs, fc]])
    second = np.block([[-fs, -fc], [fc, -fs]])
    wc, ws = np.cos(ang_i), -np.sin(ang_i)
    fh, fl = halves(np.block([[wc, ws], [-ws, wc]]))
    ih, il = halves(np.block([[wc, -ws], [ws, wc]]))
    bh, bl = halves(np.block([[fc, fs], [-fs, fc]]))
    ch, cl = halves(np.concatenate([fc, fs], axis=0))
    offsets = np.arange(sample_length).reshape(outer, inner)
    chips = offsets * chip_count // sample_length
    signs = 1 - 2 * ((offsets * 2 * chip_count // sample_length) % 2)
    starts = tuple(int(v) for v in chips[:, 0])
    within = chips - chips[:, :1]
    wide = np.concatenate([fh, fh, fl, ih, ih, il], axis=0)
    narrow = [first, second, np.cos(ang_t), -np.sin(ang_t), bh, bl,
              np.concatenate([ch, cl], axis=1), within, signs]
    narrow = np.concatenate([np.asarray(t, np.float32) for t in narrow], axis=0)
    return wide, narrow, starts


def padded(table, size):
    extra = -(-size // (table.shape[1] * table.dtype.itemsize)) - table.shape[0]
    return np.pad(table, ((0, max(extra, 0)), (0, 0)))


def split(value):
    high = value.astype(jnp.bfloat16)
    low = (value - high.astype(jnp.float32)).astype(jnp.bfloat16)
    return high, low


def mm(left, right):
    return jnp.dot(left, right, preferred_element_type=jnp.float32)


def flip(me, k, count):
    if count & (count - 1):
        return lax.rem(me + k, count)
    peer, bit = 0, 1
    while bit < count:
        peer = peer + ((me // bit + k // bit) % 2) * bit
        bit *= 2
    return peer


def back_flip(me, k, count):
    return lax.rem(me + count - k, count) if count & (count - 1) else flip(me, k, count)


def kernel(starts, outer, chip_count, cores, x_hbm, codes_hbm, dop_hbm, wide_hbm, narrow_hbm,
           power_ref, peak_ref, chips, dop_ref, wide, narrow, back,
           everyone, cpad, gath, cspec, rot, dtw, xs, spec, lagged, acc, peaks, mine,
           tab_sem, send_z, recv_z, send_twin, recv_twin, send_far, recv_far, send_tm, recv_tm,
           send_peak, recv_peak):
    inner = LANES
    tm_count, _, line, _, packed_rows, _ = everyone.shape
    dop_rows, sats = acc.shape[0], acc.shape[1]
    sample_length = outer * inner
    rows = outer // (cores * line)
    own = packed_rows // rows
    blocks = tm_count * own
    slots = spec.shape[0]
    me_tm, me_sat = lax.axis_index("tm"), lax.axis_index("sat")
    me_z, me_core = me_sat // cores, lax.rem(me_sat, cores)

    def place(z, core):
        return z * cores + core

    pairs = ((x_hbm, everyone.at[me_tm, me_core, me_z]), (codes_hbm, chips), (dop_hbm, dop_ref),
             (narrow_hbm.at[pl.ds(0, narrow.shape[0])], narrow),
             (wide_hbm.at[pl.ds(0, wide.shape[0])], wide))
    loads = [pltpu.make_async_copy(h, t, tab_sem.at[i]) for i, (h, t) in enumerate(pairs)]
    loads[0].start()

    around = [(k, c) for k in range(line) for c in range(cores) if k or c]
    far = [tm_count - 1] if tm_count > 2 else []
    near = [k for k in range(1, tm_count) if k not in far]
    barrier = pltpu.get_barrier_semaphore()
    for k, c in reversed(around):
        target = place(flip(me_z, k, line), flip(me_core, c, cores))
        pl.semaphore_signal(barrier, inc=1, device_id={"sat": target}, device_id_type=MESH)
    for k in range(1, tm_count):
        for c in range(cores):
            target = place(me_z, flip(me_core, c, cores))
            pl.semaphore_signal(
                barrier, inc=1, device_id={"tm": flip(me_tm, k, tm_count), "sat": target}, device_id_type=MESH)

    for load in loads[1:]:
        load.start()

    def pass_on(piece, sends, recvs, at, k, c):
        target = place(flip(me_z, k, line), flip(me_core, c, cores))
        return pltpu.make_async_remote_copy(
            src_ref=piece, dst_ref=piece, send_sem=sends.at[at], recv_sem=recvs.at[at],
            device_id={"sat": target}, device_id_type=MESH)

    def my_piece(z):
        return everyone.at[me_tm, me_core, z]

    def along_z(k):
        return pass_on(my_piece(me_z), send_z, recv_z, k, k, 0)

    def from_z(k):
        return pass_on(my_piece(back_flip(me_z, k, line)), send_z, recv_z, k, k, 0)

    def to_twin(k):
        return pass_on(my_piece(back_flip(me_z, k, line)), send_twin, recv_twin, k, 0, 1)

    def from_twin(k):
        piece = everyone.at[me_tm, back_flip(me_core, 1, cores), back_flip(me_z, k, line)]
        return pass_on(piece, send_twin, recv_twin, k, 0, 1)

    def far_group(k):
        return back_flip(me_tm, k, tm_count)

    def to_far(k):
        return pltpu.make_async_remote_copy(
            src_ref=my_piece(me_z), dst_ref=my_piece(me_z), send_sem=send_far.at[0], recv_sem=recv_far.at[0],
            device_id={"tm": flip(me_tm, k, tm_count)}, device_id_type=MESH)

    def from_far(k):
        piece = everyone.at[far_group(k), me_core, me_z]
        return pltpu.make_async_remote_copy(
            src_ref=piece, dst_ref=piece, send_sem=send_far.at[0], recv_sem=recv_far.at[0],
            device_id={"tm": flip(me_tm, k, tm_count)}, device_id_type=MESH)

    def spread_far(j, k, c):
        return pass_on(everyone.at[far_group(j), me_core, me_z], send_far, recv_far, k * cores + c, k, c)

    def gather_far(j, k, c):
        piece = everyone.at[far_group(j), back_flip(me_core, c, cores), back_flip(me_z, k, line)]
        return pass_on(piece, send_far, recv_far, k * cores + c, k, c)

    def relay(k, z):
        for c in range(cores):
            pltpu.make_async_remote_copy(
                src_ref=my_piece(z), dst_ref=my_piece(z), send_sem=send_tm.at[k - 1], recv_sem=recv_tm.at[k - 1],
                device_id={"tm": flip(me_tm, k, tm_count), "sat": place(me_z, flip(me_core, c, cores))},
                device_id_type=MESH).start()

    def whole_group(k, at):
        return pltpu.make_async_remote_copy(
            src_ref=everyone.at[at], dst_ref=everyone.at[at], send_sem=send_tm.at[k - 1],
            recv_sem=recv_tm.at[k - 1], device_id={"tm": flip(me_tm, k, tm_count)}, device_id_type=MESH)

    def share_peak(k):
        return pltpu.make_async_remote_copy(
            src_ref=mine, dst_ref=peaks.at[k - 1], send_sem=send_peak.at[k - 1],
            recv_sem=recv_peak.at[k - 1], device_id={"tm": flip(me_tm, k, tm_count)}, device_id_type=MESH)

    loads[0].wait()
    pl.semaphore_wait(barrier, len(around) + (tm_count - 1) * cores)
    for k in reversed(range(1, line)):
        along_z(k).start()
    for j in far:
        to_far(j).start()
    for j in near:
        relay(j, me_z)
    if cores > 1:
        to_twin(0).start()

    loads[1].wait()
    cpad[...] = jnp.zeros_like(cpad)
    cpad[0:sats, 0:chip_count] = chips[...].astype(jnp.float32)
    for n1 in range(outer):
        base = starts[n1] // LANES * LANES
        shift = starts[n1] - base
        piece = cpad[:, base:base + 2 * LANES]
        if shift:
            piece = pltpu.roll(piece, 2 * LANES - shift, 1)
        for s in range(sats):
            gath[s, n1:n1 + 1, :] = piece[s:s + 1, :LANES]
    for load in loads[2:]:
        load.wait()

    cut = [0]

    def take(count):
        cut.append(cut[-1] + count)
        return narrow[cut[-2]:cut[-1]]

    first, second = take(2 * outer), take(2 * outer)
    t_re, t_im = take(outer), take(outer)
    bh, bl = take(2 * outer).astype(jnp.bfloat16), take(2 * outer).astype(jnp.bfloat16)
    back[...] = jnp.concatenate([bh, bh, bl], axis=1)
    code = take(2 * outer).astype(jnp.bfloat16)
    within = take(outer).astype(jnp.int32)
    signs = take(outer)
    t_at = 4 * outer
    fwd_ref = wide.at[pl.ds(0, 6 * inner)]
    inv_ref = wide.at[pl.ds(6 * inner, 6 * inner)]
    scale = math.sqrt(1.0 / (float(sample_length) ** 3 * blocks))
    for s in range(sats):
        rep = jnp.take_along_axis(gath[s], within, axis=1) * signs
        rep = rep.astype(jnp.bfloat16)
        y = mm(code, jnp.concatenate([rep, rep], axis=0))
        y_re, y_im = y[:outer], y[outer:]
        z = jnp.concatenate([y_re * t_re - y_im * t_im, y_re * t_im + y_im * t_re], axis=1)
        zh, zl = split(z)
        cspec[s] = mm(jnp.concatenate([zh, zl, zh], axis=1), fwd_ref[...]) * scale

    lane = lax.broadcasted_iota(jnp.int32, (8, inner), 1)
    row_of = lax.rem(lane, outer) * inner
    base_row = me_tm * dop_rows
    turn = 2.0 * math.pi / wrap_count
    bins = lax.broadcasted_iota(jnp.int32, (8, inner), 0)
    for f0 in range(0, dop_rows, 4):
        d = jnp.zeros((8, inner), jnp.int32)
        for f in range(f0, min(f0 + 4, dop_rows)):
            d = jnp.where(lax.rem(bins, 4) == f - f0, dop_ref[base_row + f], d)
        m = (jnp.where(bins < 4, row_of, lane) * d) & (wrap_count - 1)
        angle = m.astype(jnp.float32) * turn
        cosine, sine = jnp.cos(angle), -jnp.sin(angle)
        for f in range(f0, min(f0 + 4, dop_rows)):
            i = f - f0
            c1, s1 = cosine[i:i + 1] * sample_scale, sine[i:i + 1] * sample_scale
            c2, s2 = cosine[i + 4:i + 5], sine[i + 4:i + 5]
            mh, ml = split(first * c1 + second * s1)
            rot[f] = jnp.concatenate([mh, mh, ml], axis=1)
            dtw[f, 0] = t_re * c2 - t_im * s2
            dtw[f, 1] = t_re * s2 + t_im * c2
    acc[...] = jnp.zeros_like(acc)

    for k in range(1, line):
        from_z(k).wait_recv()
        if cores > 1:
            to_twin(k).start()
        for j in near:
            relay(j, back_flip(me_z, k, line))
        if k == line // 2:
            for j in far:
                from_far(j).wait_recv()
                for n, c in around:
                    spread_far(j, n, c).start()
    if cores > 1:
        for k in range(line):
            from_twin(k).wait_recv()

    def arrive(j):
        g = back_flip(me_tm, j, tm_count)
        for blk in range(own):
            parts = [everyone[g, q % cores, q // cores, part, pl.ds(blk, rows, stride=own), :]
                     for part in range(2) for q in range(cores * line)]
            x = jnp.concatenate(parts, axis=0).astype(jnp.float32)
            xh, xl = split(x)
            at = slice(blk * inner, (blk + 1) * inner)
            xs[0:2 * outer, at] = xh
            xs[2 * outer:4 * outer, at] = xl
            xs[4 * outer:6 * outer, at] = xh

    def rotate(f):
        return mm(rot[f], xs[...])

    def spectrum(f, y):
        u_re, u_im = dtw[f, 0], dtw[f, 1]
        zs = []
        for blk in range(own):
            y_re = y[:outer, blk * inner:(blk + 1) * inner]
            y_im = y[outer:, blk * inner:(blk + 1) * inner]
            zs.append(jnp.concatenate([y_re * u_re - y_im * u_im, y_re * u_im + y_im * u_re], axis=1))
        zh, zl = split(jnp.concatenate(zs, axis=0))
        spec[f % slots] = mm(jnp.concatenate([zh, zl, zh], axis=1), fwd_ref[...])

    def cross(f):
        crosses = []
        for s in range(sats):
            k_re, k_im = cspec[s, :, :inner], cspec[s, :, inner:]
            for blk in range(own):
                s_re = spec[f % slots, blk * outer:(blk + 1) * outer, :inner]
                s_im = spec[f % slots, blk * outer:(blk + 1) * outer, inner:]
                crosses.append(jnp.concatenate(
                    [s_re * k_re + s_im * k_im, s_im * k_re - s_re * k_im], axis=1))
        ch, cl = split(jnp.concatenate(crosses, axis=0))
        lag = mm(jnp.concatenate([ch, cl, ch], axis=1), inv_ref[...])
        w_re, w_im = narrow[t_at:t_at + outer], narrow[t_at + outer:t_at + 2 * outer]
        for s in range(sats):
            for blk in range(own):
                at = (s * own + blk) * outer
                l_re, l_im = lag[at:at + outer, :inner], lag[at:at + outer, inner:]
                wh, wl = split(jnp.concatenate(
                    [l_re * w_re + l_im * w_im, l_im * w_re - l_re * w_im], axis=0))
                to = slice(blk * inner, (blk + 1) * inner)
                lagged[f % slots, s, 0:2 * outer, to] = wh
                lagged[f % slots, s, 2 * outer:4 * outer, to] = wl

    def finish(f):
        for s in range(sats):
            high, low = lagged[f % slots, s, 0:2 * outer], lagged[f % slots, s, 2 * outer:4 * outer]
            out = mm(back[...], jnp.concatenate([high, low, high], axis=0))
            o_re, o_im = out[:outer], out[outer:]
            p = o_re * o_re + o_im * o_im
            total = p[:, :inner]
            for blk in range(1, own):
                total = total + p[:, blk * inner:(blk + 1) * inner]
            acc[f, s] += total

    def step(f, forward, middle, last):
        if last:
            finish((f - 3) % dop_rows)
        if forward:
            y = rotate(f)
        if middle:
            cross((f - 1) % dop_rows)
        if forward:
            spectrum(f, y)

    def group(j, first=False):
        for f in range(dop_rows):
            if f == 0:
                arrive(j)
            step(f, True, not first or f >= 1, not first or f >= 3)

    def near_group(j, carry):
        whole_group(j, back_flip(me_tm, j, tm_count)).wait_recv()
        group(j)
        return carry

    group(0, True)
    if len(near) <= 3:
        for j in near:
            near_group(j, 0)
    else:
        lax.fori_loop(1, len(near) + 1, near_group, 0)
    for j in far:
        for n, c in around:
            gather_far(j, n, c).wait_recv()
        group(j)
    for f in range(3):
        step(f, False, f == 0, True)

    mine[...] = jnp.zeros_like(mine)
    for s in range(sats):
        top = acc[0, s]
        for f in range(1, dop_rows):
            top = jnp.maximum(top, acc[f, s])
        mine[s:s + 1, :] = jnp.max(top, axis=0, keepdims=True)
    for k in range(1, tm_count):
        share_peak(k).start()
    for f in range(dop_rows):
        for s in range(sats):
            power_ref[s, :, f, :] = acc[f, s]
    energy = jnp.zeros((8, inner), jnp.float32)
    for g in range(tm_count):
        x = everyone[g].astype(jnp.float32)
        energy = energy + jnp.sum((x * x).reshape(-1, 8, inner), axis=0)
    mean = jnp.sum(energy) * (sample_scale * sample_scale / float(blocks * sample_length))
    floor = jnp.maximum(mean, 0.25)
    for k in range(1, line):
        along_z(k).wait_send()
    if cores > 1:
        for k in range(line):
            to_twin(k).wait_send()
    for j in far:
        to_far(j).wait_send()
        for n, c in around:
            spread_far(j, n, c).wait_send()
    for k in near:
        whole_group(k, me_tm).wait_send()
    for k in range(1, tm_count):
        share_peak(k).wait()
    best = mine[...]
    for k in range(1, tm_count):
        best = jnp.maximum(best, peaks[k - 1])
    peak_ref[...] = best / floor


def stay(value):
    return pltpu.with_memory_space_constraint(value, pltpu.HBM)


def emit(power_ref, peak_ref, power_hbm, detection_hbm, detection, sems):
    copy = pltpu.make_async_copy(power_ref, power_hbm, sems.at[0])
    copy.start()
    best = jnp.max(peak_ref[...], axis=1, keepdims=True)
    shape = peak_ref.shape
    on = lax.broadcasted_iota(jnp.int32, shape, 0) == lax.broadcasted_iota(jnp.int32, shape, 1)
    row = jnp.sum(jnp.where(on, best, 0.0), axis=0)
    detection[...] = row[:detection.shape[0]]
    small = pltpu.make_async_copy(detection, detection_hbm, sems.at[1])
    small.start()
    copy.wait()
    small.wait()


def shards(samples, codes, dopplers):
    tm_count, sat_count = lax.axis_size("tm"), lax.axis_size("sat")
    own, segment = samples.shape[1], samples.shape[2]
    sample_length = segment * sat_count
    outer, rows = sample_length // LANES, segment // LANES
    sats, chip_count = codes.shape
    dop_rows = dopplers.shape[0] // tm_count
    cores = 2 if sat_count % 2 == 0 else 1
    line = sat_count // cores
    wide, narrow, starts = tables(sample_length, chip_count)
    pad = (max(starts) // LANES + 2) * LANES
    pad = max(pad, -(-chip_count // LANES) * LANES)
    peak_rows = -(-sats // 8) * 8
    slots = dop_rows if dop_rows % 2 else 2
    vm = pl.BlockSpec(memory_space=pltpu.VMEM)
    hbm = pl.BlockSpec(memory_space=pltpu.HBM)
    dma = pltpu.SemaphoreType.DMA
    packed = samples.reshape(2, own, rows, LANES).transpose(0, 2, 1, 3).reshape(2, rows * own, LANES)
    power, peak = pl.pallas_call(
        functools.partial(kernel, starts, outer, chip_count, cores),
        out_shape=(
            jax.ShapeDtypeStruct((sats, outer, dop_rows, LANES), jnp.float32),
            jax.ShapeDtypeStruct((peak_rows, LANES), jnp.float32),
        ),
        in_specs=[hbm, hbm, hbm, hbm, hbm],
        out_specs=(vm, vm),
        scratch_shapes=[
            pltpu.VMEM(codes.shape, jnp.int32),
            pltpu.SMEM(dopplers.shape, jnp.int32),
            pltpu.VMEM(wide.shape, jnp.bfloat16),
            pltpu.VMEM(narrow.shape, jnp.float32),
            pltpu.VMEM((2 * outer, 6 * outer), jnp.bfloat16),
            pltpu.VMEM((tm_count, cores, line, 2, rows * own, LANES), jnp.int32),
            pltpu.VMEM((8, pad), jnp.float32),
            pltpu.VMEM((sats, outer, LANES), jnp.float32),
            pltpu.VMEM((sats, outer, 2 * LANES), jnp.float32),
            pltpu.VMEM((dop_rows, 2 * outer, 6 * outer), jnp.bfloat16),
            pltpu.VMEM((dop_rows, 2, outer, LANES), jnp.float32),
            pltpu.VMEM((6 * outer, own * LANES), jnp.bfloat16),
            pltpu.VMEM((slots, own * outer, 2 * LANES), jnp.float32),
            pltpu.VMEM((slots, sats, 4 * outer, own * LANES), jnp.bfloat16),
            pltpu.VMEM((dop_rows, sats, outer, LANES), jnp.float32),
            pltpu.VMEM((tm_count - 1, peak_rows, LANES), jnp.float32),
            pltpu.VMEM((peak_rows, LANES), jnp.float32),
            dma((5,)),
            dma((line,)),
            dma((line,)),
            dma((line,)),
            dma((line,)),
            dma((sat_count,)),
            dma((sat_count,)),
            dma((tm_count - 1,)),
            dma((tm_count - 1,)),
            dma((tm_count - 1,)),
            dma((tm_count - 1,)),
        ],
        compiler_params=pltpu.CompilerParams(
            vmem_limit_bytes=KERNEL_BYTES, collective_id=0, has_side_effects=True),
        name="search",
    )(stay(packed), stay(codes), stay(dopplers), jnp.asarray(padded(wide, PADDING)), jnp.asarray(padded(narrow, PADDING)))
    power, detection = pl.pallas_call(
        emit,
        out_shape=(
            jax.ShapeDtypeStruct(power.shape, jnp.float32),
            jax.ShapeDtypeStruct((sats,), jnp.float32),
        ),
        in_specs=[vm, vm],
        out_specs=(hbm, hbm),
        scratch_shapes=[pltpu.VMEM((sats,), jnp.float32), dma((2,))],
        compiler_params=pltpu.CompilerParams(vmem_limit_bytes=2_000_000),
        name="emit",
    )(power, peak)
    power = power.transpose(2, 0, 1, 3).reshape(dop_rows, sats, sample_length)
    return power, detection


def solution(mesh):
    placed = (P(None, "tm", "sat"), P("sat", None), P())
    return jax.shard_map(
        shards,
        mesh=mesh,
        in_specs=placed,
        out_specs=(P("tm", "sat", None), P("sat")),
        check_vma=False,
    )
```

```python
import functools
import math

import jax
import jax.numpy as jnp
import ml_dtypes
import numpy as np
from jax import lax
from jax.experimental import pallas as pl
from jax.experimental.pallas import tpu as pltpu
from jax.sharding import PartitionSpec as P

sample_scale = 2.0 ** (-29)
wrap_count = 32768
LANES = 128
KERNEL_BYTES = 55_800_000
PADDING = 1_200_000
MESH = pl.DeviceIdType.MESH


def halves(table):
    high = table.astype(np.float32).astype(ml_dtypes.bfloat16)
    low = (table - high.astype(np.float64)).astype(np.float32).astype(ml_dtypes.bfloat16)
    return high, low


@functools.lru_cache(maxsize=None)
def tables(sample_length, chip_count, rows):
    inner = LANES
    outer = sample_length // inner
    a = np.arange(outer)
    c = np.arange(inner)
    ang_o = 2 * np.pi * (np.outer(a, a) % outer) / outer
    ang_t = 2 * np.pi * (np.outer(a, c) % sample_length) / sample_length
    ang_i = 2 * np.pi * (np.outer(c, c) % inner) / inner
    fc, fs = np.cos(ang_o), -np.sin(ang_o)
    first = np.block([[fc, -fs], [fs, fc]])
    second = np.block([[-fs, -fc], [fc, -fs]])
    wc, ws = np.cos(ang_i), -np.sin(ang_i)
    fh, fl = halves(np.block([[wc, ws], [-ws, wc]]))
    ih, il = halves(np.block([[wc, -ws], [ws, wc]]))
    full = np.block([[fc, fs], [-fs, fc]])
    half, span = outer // 2, rows // 2
    low = np.concatenate([np.arange(0, half, 2), np.arange(1, half, 2)])
    order = np.concatenate([low, low + half])
    both = np.concatenate([low, low + outer])
    spot = np.arange(outer)
    base = spot // rows * rows + spot % span * 2
    part = spot % rows // span
    column = np.concatenate([base, base + 1])
    picked = np.concatenate([part, part]) * outer + column
    first, second = first[both][:, picked], second[both][:, picked]
    keep = np.concatenate([np.arange(half), np.arange(half) + outer])
    backs = []
    for parity in range(2):
        side = np.arange(parity, outer, 2)
        bh, bl = halves(full[keep][:, np.concatenate([side, side + outer])])
        backs.append(np.concatenate([bh, bl], axis=1))
    ch, cl = halves(np.concatenate([fc[order], fs[order]], axis=0))
    offsets = np.arange(sample_length).reshape(outer, inner)
    chips = offsets * chip_count // sample_length
    signs = 1 - 2 * ((offsets * 2 * chip_count // sample_length) % 2)
    starts = tuple(int(v) for v in chips[:, 0])
    within = chips - chips[:, :1]
    wide = np.concatenate([fh, fh, fl, ih, ih, il], axis=0)
    ang_t = ang_t[order]
    narrow = [first, second, np.cos(ang_t), -np.sin(ang_t), *backs,
              np.concatenate([ch, cl], axis=1), within, signs, np.tile(column * inner, (8, 1))]
    narrow = np.concatenate([np.asarray(t, np.float32) for t in narrow], axis=0)
    return wide, narrow, starts


def padded(table, size):
    extra = -(-size // (table.shape[1] * table.dtype.itemsize)) - table.shape[0]
    return np.pad(table, ((0, max(extra, 0)), (0, 0)))


def split(value):
    high = value.astype(jnp.bfloat16)
    low = (value - high.astype(jnp.float32)).astype(jnp.bfloat16)
    return high, low


def rest(value):
    return value - value.astype(jnp.bfloat16).astype(jnp.float32)


def three(pieces, table):
    value = jnp.concatenate([jnp.concatenate(row, axis=1) for row in pieces], axis=0)
    low = jnp.concatenate([jnp.concatenate([rest(p) for p in row], axis=1) for row in pieces], axis=0)
    high, low = value.astype(jnp.bfloat16), low.astype(jnp.bfloat16)
    depth = high.shape[1]
    top, bottom = table[0:depth], table[2 * depth:3 * depth]
    return mm(high, top) + mm(low, top) + mm(high, bottom)


def mm(left, right):
    return jnp.dot(left, right, preferred_element_type=jnp.float32)


def flip(me, k, count):
    if count & (count - 1):
        return lax.rem(me + k, count)
    peer, bit = 0, 1
    while bit < count:
        peer = peer + ((me // bit + k // bit) % 2) * bit
        bit *= 2
    return peer


def back_flip(me, k, count):
    return lax.rem(me + count - k, count) if count & (count - 1) else flip(me, k, count)


def kernel(starts, outer, chip_count, cores, x_hbm, codes_hbm, dop_hbm, wide_hbm, narrow_hbm,
           power_ref, peak_ref, chips, dop_ref, wide, narrow, back,
           everyone, cpad, gath, cspec, rot, dtw, xs, spec, lagged, acc, peaks, mine,
           tab_sem, send_z, recv_z, send_twin, recv_twin, send_far, recv_far, send_tm, recv_tm,
           send_peak, recv_peak):
    inner = LANES
    tm_count, _, line, packed_rows, _ = everyone.shape
    dop_rows, sats = acc.shape[0], acc.shape[1]
    sample_length = outer * inner
    rows = outer // (cores * line)
    own = packed_rows // (2 * rows)
    half = outer // 2
    blocks = tm_count * own
    slots = spec.shape[0]
    me_tm, me_sat = lax.axis_index("tm"), lax.axis_index("sat")
    me_z, me_core = me_sat // cores, lax.rem(me_sat, cores)

    def place(z, core):
        return z * cores + core

    pairs = ((x_hbm, everyone.at[me_tm, me_core, me_z]), (codes_hbm, chips), (dop_hbm, dop_ref),
             (narrow_hbm.at[pl.ds(0, narrow.shape[0])], narrow),
             (wide_hbm.at[pl.ds(0, wide.shape[0])], wide))
    loads = [pltpu.make_async_copy(h, t, tab_sem.at[i]) for i, (h, t) in enumerate(pairs)]
    loads[0].start()

    around = [(k, c) for k in range(line) for c in range(cores) if k or c]
    far = [tm_count - 1] if tm_count > 2 else []
    near = [k for k in range(1, tm_count) if k not in far]
    barrier = pltpu.get_barrier_semaphore()
    for k, c in reversed(around):
        target = place(flip(me_z, k, line), flip(me_core, c, cores))
        pl.semaphore_signal(barrier, inc=1, device_id={"sat": target}, device_id_type=MESH)
    for k in range(1, tm_count):
        for c in range(cores):
            target = place(me_z, flip(me_core, c, cores))
            pl.semaphore_signal(
                barrier, inc=1, device_id={"tm": flip(me_tm, k, tm_count), "sat": target}, device_id_type=MESH)

    for load in loads[1:]:
        load.start()

    def pass_on(piece, sends, recvs, at, k, c):
        target = place(flip(me_z, k, line), flip(me_core, c, cores))
        return pltpu.make_async_remote_copy(
            src_ref=piece, dst_ref=piece, send_sem=sends.at[at], recv_sem=recvs.at[at],
            device_id={"sat": target}, device_id_type=MESH)

    def my_piece(z):
        return everyone.at[me_tm, me_core, z]

    def along_z(k):
        return pass_on(my_piece(me_z), send_z, recv_z, k, k, 0)

    def from_z(k):
        return pass_on(my_piece(back_flip(me_z, k, line)), send_z, recv_z, k, k, 0)

    def to_twin(k):
        return pass_on(my_piece(back_flip(me_z, k, line)), send_twin, recv_twin, k, 0, 1)

    def from_twin(k):
        piece = everyone.at[me_tm, back_flip(me_core, 1, cores), back_flip(me_z, k, line)]
        return pass_on(piece, send_twin, recv_twin, k, 0, 1)

    def far_group(k):
        return back_flip(me_tm, k, tm_count)

    def to_far(k):
        return pltpu.make_async_remote_copy(
            src_ref=my_piece(me_z), dst_ref=my_piece(me_z), send_sem=send_far.at[0], recv_sem=recv_far.at[0],
            device_id={"tm": flip(me_tm, k, tm_count)}, device_id_type=MESH)

    def from_far(k):
        piece = everyone.at[far_group(k), me_core, me_z]
        return pltpu.make_async_remote_copy(
            src_ref=piece, dst_ref=piece, send_sem=send_far.at[0], recv_sem=recv_far.at[0],
            device_id={"tm": flip(me_tm, k, tm_count)}, device_id_type=MESH)

    def spread_far(j, k, c):
        return pass_on(everyone.at[far_group(j), me_core, me_z], send_far, recv_far, k * cores + c, k, c)

    def gather_far(j, k, c):
        piece = everyone.at[far_group(j), back_flip(me_core, c, cores), back_flip(me_z, k, line)]
        return pass_on(piece, send_far, recv_far, k * cores + c, k, c)

    def relay(k, z):
        for c in range(cores):
            pltpu.make_async_remote_copy(
                src_ref=my_piece(z), dst_ref=my_piece(z), send_sem=send_tm.at[k - 1], recv_sem=recv_tm.at[k - 1],
                device_id={"tm": flip(me_tm, k, tm_count), "sat": place(me_z, flip(me_core, c, cores))},
                device_id_type=MESH).start()

    def whole_group(k, at):
        return pltpu.make_async_remote_copy(
            src_ref=everyone.at[at], dst_ref=everyone.at[at], send_sem=send_tm.at[k - 1],
            recv_sem=recv_tm.at[k - 1], device_id={"tm": flip(me_tm, k, tm_count)}, device_id_type=MESH)

    def share_peak(k):
        return pltpu.make_async_remote_copy(
            src_ref=mine, dst_ref=peaks.at[k - 1], send_sem=send_peak.at[k - 1],
            recv_sem=recv_peak.at[k - 1], device_id={"tm": flip(me_tm, k, tm_count)}, device_id_type=MESH)

    loads[0].wait()
    pl.semaphore_wait(barrier, len(around) + (tm_count - 1) * cores)
    for k in reversed(range(1, line)):
        along_z(k).start()
    for j in far:
        to_far(j).start()
    for j in near:
        relay(j, me_z)
    if cores > 1:
        to_twin(0).start()

    loads[1].wait()
    cpad[...] = jnp.zeros_like(cpad)
    cpad[0:sats, 0:chip_count] = chips[...].astype(jnp.float32)
    for n1 in range(outer):
        base = starts[n1] // LANES * LANES
        shift = starts[n1] - base
        piece = cpad[:, base:base + 2 * LANES]
        if shift:
            piece = pltpu.roll(piece, 2 * LANES - shift, 1)
        for s in range(sats):
            gath[s, n1:n1 + 1, :] = piece[s:s + 1, :LANES]
    for load in loads[2:]:
        load.wait()

    cut = [0]

    def take(count):
        cut.append(cut[-1] + count)
        return narrow[cut[-2]:cut[-1]]

    first, second = take(outer), take(outer)
    t_re, t_im = take(outer), take(outer)
    for parity in range(2):
        table = take(outer)
        bh, bl = table[:, :outer], table[:, outer:]
        back[parity] = jnp.concatenate([bh, bh, bl], axis=1).astype(jnp.bfloat16)
    code = take(2 * outer).astype(jnp.bfloat16)
    within = take(outer).astype(jnp.int32)
    signs = take(outer)
    row_of = take(8).astype(jnp.int32)
    t_at = 2 * outer
    fwd_ref = wide.at[pl.ds(0, 6 * inner)]
    inv_ref = wide.at[pl.ds(6 * inner, 6 * inner)]
    scale = math.sqrt(1.0 / (float(sample_length) ** 3 * blocks))
    for s in range(sats):
        rep = jnp.take_along_axis(gath[s], within, axis=1) * signs
        rep = rep.astype(jnp.bfloat16)
        y = mm(code, jnp.concatenate([rep, rep], axis=0))
        y_re, y_im = y[:outer], y[outer:]
        z = jnp.concatenate([y_re * t_re - y_im * t_im, y_re * t_im + y_im * t_re], axis=1)
        zh, zl = split(z)
        cspec[s] = mm(jnp.concatenate([zh, zl, zh], axis=1), fwd_ref[...]) * scale

    lane = lax.broadcasted_iota(jnp.int32, (8, inner), 1)
    base_row = me_tm * dop_rows
    turn = 2.0 * math.pi / wrap_count
    bins = lax.broadcasted_iota(jnp.int32, (8, inner), 0)
    for f0 in range(0, dop_rows, 4):
        d = jnp.zeros((8, inner), jnp.int32)
        for f in range(f0, min(f0 + 4, dop_rows)):
            d = jnp.where(lax.rem(bins, 4) == f - f0, dop_ref[base_row + f], d)
        m = (jnp.where(bins < 4, row_of, lane) * d) & (wrap_count - 1)
        angle = m.astype(jnp.float32) * turn
        cosine, sine = jnp.cos(angle), -jnp.sin(angle)
        for f in range(f0, min(f0 + 4, dop_rows)):
            i = f - f0
            c1, s1 = cosine[i:i + 1] * sample_scale, sine[i:i + 1] * sample_scale
            c2, s2 = cosine[i + 4:i + 5], sine[i + 4:i + 5]
            mix = first * c1 + second * s1
            low = mix - mix.astype(jnp.bfloat16).astype(jnp.float32)
            for parity in range(2):
                at = slice(parity * outer, (parity + 1) * outer)
                rot[f, parity] = jnp.concatenate([mix[:, at], mix[:, at], low[:, at]], axis=1).astype(jnp.bfloat16)
            dtw[f, 0] = t_re * c2 - t_im * s2
            dtw[f, 1] = t_re * s2 + t_im * c2
    acc[...] = jnp.zeros_like(acc)

    for k in range(1, line):
        from_z(k).wait_recv()
        if cores > 1:
            to_twin(k).start()
        for j in near:
            relay(j, back_flip(me_z, k, line))
        if k == line // 2:
            for j in far:
                from_far(j).wait_recv()
                for n, c in around:
                    spread_far(j, n, c).start()
    if cores > 1:
        for k in range(line):
            from_twin(k).wait_recv()

    def arrive(j):
        g = back_flip(me_tm, j, tm_count)
        for parity in range(2):
            cols = []
            for blk in range(own):
                parts = [everyone[g, q % cores, q // cores, pl.ds(parity * own + blk, rows, stride=2 * own), :]
                         for q in range(cores * line)]
                cols.append(jnp.concatenate(parts, axis=0))
            xh, xl = split(jnp.concatenate(cols, axis=1).astype(jnp.float32))
            xs[parity, 0:outer] = xh
            xs[parity, outer:2 * outer] = xl

    def rotate(f):
        sides = []
        for parity in range(2):
            high, low = xs[parity, 0:outer], xs[parity, outer:2 * outer]
            sides.append(mm(rot[f, parity], jnp.concatenate([high, low, high], axis=0)))
        return sides

    def spectrum(f, sides):
        u_re, u_im = dtw[f, 0], dtw[f, 1]
        plus, minus = sides[0] + sides[1], sides[0] - sides[1]
        zs = []
        for blk in range(own):
            at = slice(blk * inner, (blk + 1) * inner)
            y_re = jnp.concatenate([plus[:half, at], minus[:half, at]], axis=0)
            y_im = jnp.concatenate([plus[half:, at], minus[half:, at]], axis=0)
            zs.append((y_re * u_re - y_im * u_im, y_re * u_im + y_im * u_re))
        spec[f % slots] = three(zs, fwd_ref)

    def cross(f, s):
        crosses = []
        k_re, k_im = cspec[s, :, :inner], cspec[s, :, inner:]
        for blk in range(own):
            s_re = spec[f % slots, blk * outer:(blk + 1) * outer, :inner]
            s_im = spec[f % slots, blk * outer:(blk + 1) * outer, inner:]
            crosses.append((s_re * k_re + s_im * k_im, s_im * k_re - s_re * k_im))
        lag = three(crosses, inv_ref)
        w_re, w_im = narrow[t_at:t_at + outer], narrow[t_at + outer:t_at + 2 * outer]
        quarter = outer // 4
        cols = ([], [])
        for blk in range(own):
            at = blk * outer
            l_re, l_im = lag[at:at + outer, :inner], lag[at:at + outer, inner:]
            v_re, v_im = l_re * w_re + l_im * w_im, l_im * w_re - l_re * w_im
            for parity in range(2):
                one = slice(parity * quarter, (parity + 1) * quarter)
                two = slice(half + parity * quarter, half + (parity + 1) * quarter)
                cols[parity].append(jnp.concatenate([v_re[one], v_re[two], v_im[one], v_im[two]], axis=0))
        for parity in range(2):
            wh, wl = split(jnp.concatenate(cols[parity], axis=1))
            lagged[f % slots, s, parity, 0:outer] = wh
            lagged[f % slots, s, parity, outer:2 * outer] = wl

    def finish(f, s):
        sides = []
        for parity in range(2):
            high, low = lagged[f % slots, s, parity, 0:outer], lagged[f % slots, s, parity, outer:2 * outer]
            sides.append(mm(back[parity], jnp.concatenate([high, low, high], axis=0)))
        for at, out in ((0, sides[0] + sides[1]), (half, sides[0] - sides[1])):
            o_re, o_im = out[:half], out[half:]
            p = o_re * o_re + o_im * o_im
            total = p[:, :inner]
            for blk in range(1, own):
                total = total + p[:, blk * inner:(blk + 1) * inner]
            acc[f, s, at:at + half] += total

    def step(f, forward, middle, last):
        for s in range(sats):
            if last:
                finish((f - 3) % dop_rows, s)
            if s == 0 and forward:
                y = rotate(f)
            if middle:
                cross((f - 1) % dop_rows, s)
            if s == max(sats - 2, 0) and forward:
                spectrum(f, y)

    def group(j, first=False):
        for f in range(dop_rows):
            if f == 0:
                arrive(j)
            step(f, True, not first or f >= 1, not first or f >= 3)

    def await_near(j):
        whole_group(j, back_flip(me_tm, j, tm_count)).wait_recv()

    def await_far(j):
        for n, c in around:
            gather_far(j, n, c).wait_recv()

    def near_group(j, carry):
        await_near(j)
        group(j)
        return carry

    group(0, True)
    if len(near) <= 3:
        for j in near:
            await_near(j)
            if j == len(near):
                for k in far:
                    await_far(k)
            group(j)
    else:
        lax.fori_loop(1, len(near) + 1, near_group, 0)
        for j in far:
            await_far(j)
    for j in far:
        group(j)
    for f in range(3):
        step(f, False, f == 0, True)

    mine[...] = jnp.zeros_like(mine)
    for s in range(sats):
        top = acc[0, s]
        for f in range(1, dop_rows):
            top = jnp.maximum(top, acc[f, s])
        mine[s:s + 1, :] = jnp.max(top, axis=0, keepdims=True)
    for k in range(1, tm_count):
        share_peak(k).start()
    for f in range(dop_rows):
        for s in range(sats):
            power_ref[s, :, f, :] = acc[f, s]
    energy = jnp.zeros((8, inner), jnp.float32)
    for g in range(tm_count):
        x = everyone[g].astype(jnp.float32)
        energy = energy + jnp.sum((x * x).reshape(-1, 8, inner), axis=0)
    mean = jnp.sum(energy) * (sample_scale * sample_scale / float(blocks * sample_length))
    floor = jnp.maximum(mean, 0.25)
    for k in range(1, line):
        along_z(k).wait_send()
    if cores > 1:
        for k in range(line):
            to_twin(k).wait_send()
    for j in far:
        to_far(j).wait_send()
        for n, c in around:
            spread_far(j, n, c).wait_send()
    for k in near:
        whole_group(k, me_tm).wait_send()
    for k in range(1, tm_count):
        share_peak(k).wait()
    best = mine[...]
    for k in range(1, tm_count):
        best = jnp.maximum(best, peaks[k - 1])
    peak_ref[...] = best / floor


def stay(value):
    return pltpu.with_memory_space_constraint(value, pltpu.HBM)


def emit(power_ref, peak_ref, power_hbm, detection_hbm, detection, sems):
    copy = pltpu.make_async_copy(power_ref, power_hbm, sems.at[0])
    copy.start()
    best = jnp.max(peak_ref[...], axis=1, keepdims=True)
    shape = peak_ref.shape
    on = lax.broadcasted_iota(jnp.int32, shape, 0) == lax.broadcasted_iota(jnp.int32, shape, 1)
    row = jnp.sum(jnp.where(on, best, 0.0), axis=0)
    detection[...] = row[:detection.shape[0]]
    small = pltpu.make_async_copy(detection, detection_hbm, sems.at[1])
    small.start()
    copy.wait()
    small.wait()


def shards(samples, codes, dopplers):
    tm_count, sat_count = lax.axis_size("tm"), lax.axis_size("sat")
    own, segment = samples.shape[1], samples.shape[2]
    sample_length = segment * sat_count
    outer, rows = sample_length // LANES, segment // LANES
    sats, chip_count = codes.shape
    dop_rows = dopplers.shape[0] // tm_count
    cores = 2 if sat_count % 2 == 0 else 1
    line = sat_count // cores
    wide, narrow, starts = tables(sample_length, chip_count, rows)
    pad = (max(starts) // LANES + 2) * LANES
    pad = max(pad, -(-chip_count // LANES) * LANES)
    peak_rows = -(-sats // 8) * 8
    slots = dop_rows if dop_rows % 2 else 2
    vm = pl.BlockSpec(memory_space=pltpu.VMEM)
    hbm = pl.BlockSpec(memory_space=pltpu.HBM)
    dma = pltpu.SemaphoreType.DMA
    packed = samples.reshape(2, own, rows, LANES).transpose(0, 2, 1, 3).reshape(2 * rows * own, LANES)
    power, peak = pl.pallas_call(
        functools.partial(kernel, starts, outer, chip_count, cores),
        out_shape=(
            jax.ShapeDtypeStruct((sats, outer, dop_rows, LANES), jnp.float32),
            jax.ShapeDtypeStruct((peak_rows, LANES), jnp.float32),
        ),
        in_specs=[hbm, hbm, hbm, hbm, hbm],
        out_specs=(vm, vm),
        scratch_shapes=[
            pltpu.VMEM(codes.shape, jnp.int32),
            pltpu.SMEM(dopplers.shape, jnp.int32),
            pltpu.VMEM(wide.shape, jnp.bfloat16),
            pltpu.VMEM(narrow.shape, jnp.float32),
            pltpu.VMEM((2, outer, 3 * outer), jnp.bfloat16),
            pltpu.VMEM((tm_count, cores, line, 2 * rows * own, LANES), jnp.int32),
            pltpu.VMEM((8, pad), jnp.float32),
            pltpu.VMEM((sats, outer, LANES), jnp.float32),
            pltpu.VMEM((sats, outer, 2 * LANES), jnp.float32),
            pltpu.VMEM((dop_rows, 2, outer, 3 * outer), jnp.bfloat16),
            pltpu.VMEM((dop_rows, 2, outer, LANES), jnp.float32),
            pltpu.VMEM((2, 2 * outer, own * LANES), jnp.bfloat16),
            pltpu.VMEM((slots, own * outer, 2 * LANES), jnp.float32),
            pltpu.VMEM((slots, sats, 2, 2 * outer, own * LANES), jnp.bfloat16),
            pltpu.VMEM((dop_rows, sats, outer, LANES), jnp.float32),
            pltpu.VMEM((tm_count - 1, peak_rows, LANES), jnp.float32),
            pltpu.VMEM((peak_rows, LANES), jnp.float32),
            dma((5,)),
            dma((line,)),
            dma((line,)),
            dma((line,)),
            dma((line,)),
            dma((sat_count,)),
            dma((sat_count,)),
            dma((tm_count - 1,)),
            dma((tm_count - 1,)),
            dma((tm_count - 1,)),
            dma((tm_count - 1,)),
        ],
        compiler_params=pltpu.CompilerParams(
            vmem_limit_bytes=KERNEL_BYTES, collective_id=0, has_side_effects=True),
        name="search",
    )(stay(packed), stay(codes), stay(dopplers), jnp.asarray(padded(wide, PADDING)), jnp.asarray(padded(narrow, PADDING)))
    power, detection = pl.pallas_call(
        emit,
        out_shape=(
            jax.ShapeDtypeStruct(power.shape, jnp.float32),
            jax.ShapeDtypeStruct((sats,), jnp.float32),
        ),
        in_specs=[vm, vm],
        out_specs=(hbm, hbm),
        scratch_shapes=[pltpu.VMEM((sats,), jnp.float32), dma((2,))],
        compiler_params=pltpu.CompilerParams(vmem_limit_bytes=2_000_000),
        name="emit",
    )(power, peak)
    power = power.transpose(2, 0, 1, 3).reshape(dop_rows, sats, sample_length)
    return power, detection


def solution(mesh):
    placed = (P(None, "tm", "sat"), P("sat", None), P())
    return jax.shard_map(
        shards,
        mesh=mesh,
        in_specs=placed,
        out_specs=(P("tm", "sat", None), P("sat")),
        check_vma=False,
    )
```

```python
import functools
import math

import jax
import jax.numpy as jnp
import ml_dtypes
import numpy as np
from jax import lax
from jax.experimental import pallas as pl
from jax.experimental.pallas import tpu as pltpu
from jax.sharding import PartitionSpec as P

sample_scale = 2.0 ** (-29)
wrap_count = 32768
LANES = 128
KERNEL_BYTES = 55_800_000
PADDING = 1_200_000
MESH = pl.DeviceIdType.MESH


def halves(table):
    high = table.astype(np.float32).astype(ml_dtypes.bfloat16)
    low = (table - high.astype(np.float64)).astype(np.float32).astype(ml_dtypes.bfloat16)
    return high, low


@functools.lru_cache(maxsize=None)
def tables(sample_length, chip_count, rows):
    inner = LANES
    outer = sample_length // inner
    a = np.arange(outer)
    c = np.arange(inner)
    ang_o = 2 * np.pi * (np.outer(a, a) % outer) / outer
    ang_t = 2 * np.pi * (np.outer(a, c) % sample_length) / sample_length
    ang_i = 2 * np.pi * (np.outer(c, c) % inner) / inner
    fc, fs = np.cos(ang_o), -np.sin(ang_o)
    first = np.block([[fc, -fs], [fs, fc]])
    second = np.block([[-fs, -fc], [fc, -fs]])
    wc, ws = np.cos(ang_i), -np.sin(ang_i)
    fh, fl = halves(np.block([[wc, ws], [-ws, wc]]))
    ih, il = halves(np.block([[wc, -ws], [ws, wc]]))
    full = np.block([[fc, fs], [-fs, fc]])
    half, span = outer // 2, rows // 2
    low = np.concatenate([np.arange(0, half, 2), np.arange(1, half, 2)])
    order = np.concatenate([low, low + half])
    both = np.concatenate([low, low + outer])
    spot = np.arange(outer)
    base = spot // rows * rows + spot % span * 2
    part = spot % rows // span
    column = np.concatenate([base, base + 1])
    picked = np.concatenate([part, part]) * outer + column
    first, second = first[both][:, picked], second[both][:, picked]
    keep = np.concatenate([np.arange(half), np.arange(half) + outer])
    backs = []
    for parity in range(2):
        side = np.arange(parity, outer, 2)
        bh, bl = halves(full[keep][:, np.concatenate([side, side + outer])])
        backs.append(np.concatenate([bh, bl], axis=1))
    ch, cl = halves(np.concatenate([fc[order], fs[order]], axis=0))
    offsets = np.arange(sample_length).reshape(outer, inner)
    chips = offsets * chip_count // sample_length
    signs = 1 - 2 * ((offsets * 2 * chip_count // sample_length) % 2)
    starts = tuple(int(v) for v in chips[:, 0])
    within = chips - chips[:, :1]
    wide = np.concatenate([fh, fh, fl, ih, ih, il], axis=0)
    ang_t = ang_t[order]
    narrow = [first, second, np.cos(ang_t), -np.sin(ang_t), *backs,
              np.concatenate([ch, cl], axis=1), within, signs, np.tile(column * inner, (8, 1))]
    narrow = np.concatenate([np.asarray(t, np.float32) for t in narrow], axis=0)
    return wide, narrow, starts


def padded(table, size):
    extra = -(-size // (table.shape[1] * table.dtype.itemsize)) - table.shape[0]
    return np.pad(table, ((0, max(extra, 0)), (0, 0)))


def split(value):
    high = value.astype(jnp.bfloat16)
    low = (value - high.astype(jnp.float32)).astype(jnp.bfloat16)
    return high, low


def rest(value):
    return value - value.astype(jnp.bfloat16).astype(jnp.float32)


def three(pieces, table):
    value = jnp.concatenate([jnp.concatenate(row, axis=1) for row in pieces], axis=0)
    low = jnp.concatenate([jnp.concatenate([rest(p) for p in row], axis=1) for row in pieces], axis=0)
    high, low = value.astype(jnp.bfloat16), low.astype(jnp.bfloat16)
    depth = high.shape[1]
    top, bottom = table[0:depth], table[2 * depth:3 * depth]
    count = high.shape[0]
    pair = mm(jnp.concatenate([high, low], axis=0), top)
    return pair[:count] + (pair[count:] + mm(high, bottom))


def mm(left, right):
    return jnp.dot(left, right, preferred_element_type=jnp.float32)


def flip(me, k, count):
    if count & (count - 1):
        return lax.rem(me + k, count)
    peer, bit = 0, 1
    while bit < count:
        peer = peer + ((me // bit + k // bit) % 2) * bit
        bit *= 2
    return peer


def back_flip(me, k, count):
    return lax.rem(me + count - k, count) if count & (count - 1) else flip(me, k, count)


def kernel(starts, outer, chip_count, cores, x_hbm, codes_hbm, dop_hbm, wide_hbm, narrow_hbm,
           power_ref, peak_ref, chips, dop_ref, wide, narrow, back,
           everyone, cpad, gath, cspec, rot, dtw, xs, spec, lagged, acc, peaks, mine,
           tab_sem, send_z, recv_z, send_twin, recv_twin, send_far, recv_far, send_tm, recv_tm,
           send_peak, recv_peak):
    inner = LANES
    tm_count, _, line, packed_rows, _ = everyone.shape
    dop_rows, sats = acc.shape[0], acc.shape[1]
    sample_length = outer * inner
    rows = outer // (cores * line)
    own = packed_rows // (2 * rows)
    half = outer // 2
    blocks = tm_count * own
    slots = spec.shape[0]
    me_tm, me_sat = lax.axis_index("tm"), lax.axis_index("sat")
    me_z, me_core = me_sat // cores, lax.rem(me_sat, cores)

    def place(z, core):
        return z * cores + core

    pairs = ((x_hbm, everyone.at[me_tm, me_core, me_z]), (codes_hbm, chips), (dop_hbm, dop_ref),
             (narrow_hbm.at[pl.ds(0, narrow.shape[0])], narrow),
             (wide_hbm.at[pl.ds(0, wide.shape[0])], wide))
    loads = [pltpu.make_async_copy(h, t, tab_sem.at[i]) for i, (h, t) in enumerate(pairs)]
    loads[0].start()

    around = [(k, c) for k in range(line) for c in range(cores) if k or c]
    far = [tm_count - 1] if tm_count > 2 else []
    near = [k for k in range(1, tm_count) if k not in far]
    barrier = pltpu.get_barrier_semaphore()
    for k, c in reversed(around):
        target = place(flip(me_z, k, line), flip(me_core, c, cores))
        pl.semaphore_signal(barrier, inc=1, device_id={"sat": target}, device_id_type=MESH)
    for k in range(1, tm_count):
        for c in range(cores):
            target = place(me_z, flip(me_core, c, cores))
            pl.semaphore_signal(
                barrier, inc=1, device_id={"tm": flip(me_tm, k, tm_count), "sat": target}, device_id_type=MESH)

    for load in loads[1:]:
        load.start()

    def pass_on(piece, sends, recvs, at, k, c):
        target = place(flip(me_z, k, line), flip(me_core, c, cores))
        return pltpu.make_async_remote_copy(
            src_ref=piece, dst_ref=piece, send_sem=sends.at[at], recv_sem=recvs.at[at],
            device_id={"sat": target}, device_id_type=MESH)

    def my_piece(z):
        return everyone.at[me_tm, me_core, z]

    def along_z(k):
        return pass_on(my_piece(me_z), send_z, recv_z, k, k, 0)

    def from_z(k):
        return pass_on(my_piece(back_flip(me_z, k, line)), send_z, recv_z, k, k, 0)

    def to_twin(k):
        return pass_on(my_piece(back_flip(me_z, k, line)), send_twin, recv_twin, k, 0, 1)

    def from_twin(k):
        piece = everyone.at[me_tm, back_flip(me_core, 1, cores), back_flip(me_z, k, line)]
        return pass_on(piece, send_twin, recv_twin, k, 0, 1)

    def far_group(k):
        return back_flip(me_tm, k, tm_count)

    def to_far(k):
        return pltpu.make_async_remote_copy(
            src_ref=my_piece(me_z), dst_ref=my_piece(me_z), send_sem=send_far.at[0], recv_sem=recv_far.at[0],
            device_id={"tm": flip(me_tm, k, tm_count)}, device_id_type=MESH)

    def from_far(k):
        piece = everyone.at[far_group(k), me_core, me_z]
        return pltpu.make_async_remote_copy(
            src_ref=piece, dst_ref=piece, send_sem=send_far.at[0], recv_sem=recv_far.at[0],
            device_id={"tm": flip(me_tm, k, tm_count)}, device_id_type=MESH)

    def spread_far(j, k, c):
        return pass_on(everyone.at[far_group(j), me_core, me_z], send_far, recv_far, k * cores + c, k, c)

    def gather_far(j, k, c):
        piece = everyone.at[far_group(j), back_flip(me_core, c, cores), back_flip(me_z, k, line)]
        return pass_on(piece, send_far, recv_far, k * cores + c, k, c)

    def relay(k, z):
        for c in range(cores):
            pltpu.make_async_remote_copy(
                src_ref=my_piece(z), dst_ref=my_piece(z), send_sem=send_tm.at[k - 1], recv_sem=recv_tm.at[k - 1],
                device_id={"tm": flip(me_tm, k, tm_count), "sat": place(me_z, flip(me_core, c, cores))},
                device_id_type=MESH).start()

    def whole_group(k, at):
        return pltpu.make_async_remote_copy(
            src_ref=everyone.at[at], dst_ref=everyone.at[at], send_sem=send_tm.at[k - 1],
            recv_sem=recv_tm.at[k - 1], device_id={"tm": flip(me_tm, k, tm_count)}, device_id_type=MESH)

    def share_peak(k):
        return pltpu.make_async_remote_copy(
            src_ref=mine, dst_ref=peaks.at[k - 1], send_sem=send_peak.at[k - 1],
            recv_sem=recv_peak.at[k - 1], device_id={"tm": flip(me_tm, k, tm_count)}, device_id_type=MESH)

    loads[0].wait()
    pl.semaphore_wait(barrier, len(around) + (tm_count - 1) * cores)
    for k in reversed(range(1, line)):
        along_z(k).start()
    for j in far:
        to_far(j).start()
    for j in near:
        relay(j, me_z)
    if cores > 1:
        to_twin(0).start()

    loads[1].wait()
    cpad[...] = jnp.zeros_like(cpad)
    cpad[0:sats, 0:chip_count] = chips[...].astype(jnp.float32)
    for n1 in range(outer):
        base = starts[n1] // LANES * LANES
        shift = starts[n1] - base
        piece = cpad[:, base:base + 2 * LANES]
        if shift:
            piece = pltpu.roll(piece, 2 * LANES - shift, 1)
        for s in range(sats):
            gath[s, n1:n1 + 1, :] = piece[s:s + 1, :LANES]
    for load in loads[2:]:
        load.wait()

    cut = [0]

    def take(count):
        cut.append(cut[-1] + count)
        return narrow[cut[-2]:cut[-1]]

    first, second = take(outer), take(outer)
    t_re, t_im = take(outer), take(outer)
    for parity in range(2):
        table = take(outer)
        bh, bl = table[:, :outer], table[:, outer:]
        back[parity] = jnp.concatenate([bh, bh, bl], axis=1).astype(jnp.bfloat16)
    code = take(2 * outer).astype(jnp.bfloat16)
    within = take(outer).astype(jnp.int32)
    signs = take(outer)
    row_of = take(8).astype(jnp.int32)
    t_at = 2 * outer
    fwd_ref = wide.at[pl.ds(0, 6 * inner)]
    inv_ref = wide.at[pl.ds(6 * inner, 6 * inner)]
    scale = math.sqrt(1.0 / (float(sample_length) ** 3 * blocks))
    for s in range(sats):
        rep = jnp.take_along_axis(gath[s], within, axis=1) * signs
        rep = rep.astype(jnp.bfloat16)
        y = mm(code, jnp.concatenate([rep, rep], axis=0))
        y_re, y_im = y[:outer], y[outer:]
        z = jnp.concatenate([y_re * t_re - y_im * t_im, y_re * t_im + y_im * t_re], axis=1)
        zh, zl = split(z)
        cspec[s] = mm(jnp.concatenate([zh, zl, zh], axis=1), fwd_ref[...]) * scale

    lane = lax.broadcasted_iota(jnp.int32, (8, inner), 1)
    base_row = me_tm * dop_rows
    turn = 2.0 * math.pi / wrap_count
    bins = lax.broadcasted_iota(jnp.int32, (8, inner), 0)
    for f0 in range(0, dop_rows, 4):
        d = jnp.zeros((8, inner), jnp.int32)
        for f in range(f0, min(f0 + 4, dop_rows)):
            d = jnp.where(lax.rem(bins, 4) == f - f0, dop_ref[base_row + f], d)
        m = (jnp.where(bins < 4, row_of, lane) * d) & (wrap_count - 1)
        angle = m.astype(jnp.float32) * turn
        cosine, sine = jnp.cos(angle), -jnp.sin(angle)
        for f in range(f0, min(f0 + 4, dop_rows)):
            i = f - f0
            c1, s1 = cosine[i:i + 1] * sample_scale, sine[i:i + 1] * sample_scale
            c2, s2 = cosine[i + 4:i + 5], sine[i + 4:i + 5]
            mix = first * c1 + second * s1
            low = mix - mix.astype(jnp.bfloat16).astype(jnp.float32)
            for parity in range(2):
                at = slice(parity * outer, (parity + 1) * outer)
                rot[f, parity] = jnp.concatenate([mix[:, at], mix[:, at], low[:, at]], axis=1).astype(jnp.bfloat16)
            dtw[f, 0] = t_re * c2 - t_im * s2
            dtw[f, 1] = t_re * s2 + t_im * c2
    acc[...] = jnp.zeros_like(acc)

    for k in range(1, line):
        from_z(k).wait_recv()
        if cores > 1:
            to_twin(k).start()
        for j in near:
            relay(j, back_flip(me_z, k, line))
        if k == line // 2:
            for j in far:
                from_far(j).wait_recv()
                for n, c in around:
                    spread_far(j, n, c).start()
    if cores > 1:
        for k in range(line):
            from_twin(k).wait_recv()

    def arrive(j):
        g = back_flip(me_tm, j, tm_count)
        for parity in range(2):
            cols = []
            for blk in range(own):
                parts = [everyone[g, q % cores, q // cores, pl.ds(parity * own + blk, rows, stride=2 * own), :]
                         for q in range(cores * line)]
                cols.append(jnp.concatenate(parts, axis=0))
            xh, xl = split(jnp.concatenate(cols, axis=1).astype(jnp.float32))
            xs[parity, 0:outer] = xh
            xs[parity, outer:2 * outer] = xl

    def rotate(f):
        sides = []
        for parity in range(2):
            high, low = xs[parity, 0:outer], xs[parity, outer:2 * outer]
            sides.append(mm(rot[f, parity], jnp.concatenate([high, low, high], axis=0)))
        return sides

    def spectrum(f, sides):
        u_re, u_im = dtw[f, 0], dtw[f, 1]
        plus, minus = sides[0] + sides[1], sides[0] - sides[1]
        zs = []
        for blk in range(own):
            at = slice(blk * inner, (blk + 1) * inner)
            y_re = jnp.concatenate([plus[:half, at], minus[:half, at]], axis=0)
            y_im = jnp.concatenate([plus[half:, at], minus[half:, at]], axis=0)
            zs.append((y_re * u_re - y_im * u_im, y_re * u_im + y_im * u_re))
        spec[f % slots] = three(zs, fwd_ref)

    def cross(f, s):
        crosses = []
        k_re, k_im = cspec[s, :, :inner], cspec[s, :, inner:]
        for blk in range(own):
            s_re = spec[f % slots, blk * outer:(blk + 1) * outer, :inner]
            s_im = spec[f % slots, blk * outer:(blk + 1) * outer, inner:]
            crosses.append((s_re * k_re + s_im * k_im, s_im * k_re - s_re * k_im))
        lag = three(crosses, inv_ref)
        w_re, w_im = narrow[t_at:t_at + outer], narrow[t_at + outer:t_at + 2 * outer]
        quarter = outer // 4
        cols = ([], [])
        for blk in range(own):
            at = blk * outer
            l_re, l_im = lag[at:at + outer, :inner], lag[at:at + outer, inner:]
            v_re, v_im = l_re * w_re + l_im * w_im, l_im * w_re - l_re * w_im
            for parity in range(2):
                one = slice(parity * quarter, (parity + 1) * quarter)
                two = slice(half + parity * quarter, half + (parity + 1) * quarter)
                cols[parity].append(jnp.concatenate([v_re[one], v_re[two], v_im[one], v_im[two]], axis=0))
        for parity in range(2):
            wh, wl = split(jnp.concatenate(cols[parity], axis=1))
            lagged[f % slots, s, parity, 0:outer] = wh
            lagged[f % slots, s, parity, outer:2 * outer] = wl

    def finish(f, s):
        sides = []
        for parity in range(2):
            high, low = lagged[f % slots, s, parity, 0:outer], lagged[f % slots, s, parity, outer:2 * outer]
            sides.append(mm(back[parity], jnp.concatenate([high, low, high], axis=0)))
        for at, out in ((0, sides[0] + sides[1]), (half, sides[0] - sides[1])):
            o_re, o_im = out[:half], out[half:]
            p = o_re * o_re + o_im * o_im
            total = p[:, :inner]
            for blk in range(1, own):
                total = total + p[:, blk * inner:(blk + 1) * inner]
            acc[f, s, at:at + half] += total

    def step(f, forward, middle, last):
        if forward:
            y = rotate(f)
        for s in range(sats):
            if middle:
                cross((f - 1) % dop_rows, s)
            if s == max(sats - 2, 0) and forward:
                spectrum(f, y)
            if last:
                finish((f - 2) % dop_rows, s)

    def group(j, first=False):
        for f in range(dop_rows):
            if f == 0:
                arrive(j)
            step(f, True, not first or f >= 1, not first or f >= 2)

    def await_near(j):
        whole_group(j, back_flip(me_tm, j, tm_count)).wait_recv()

    def near_group(j, carry):
        await_near(j)
        group(j)
        return carry

    group(0, True)
    if len(near) <= 3:
        for j in near:
            await_near(j)
        for j in near:
            group(j)
    else:
        lax.fori_loop(1, len(near) + 1, near_group, 0)
    for j in far:
        for n, c in around:
            gather_far(j, n, c).wait_recv()
        group(j)
    for f in range(2):
        step(f, False, f == 0, True)

    mine[...] = jnp.zeros_like(mine)
    for s in range(sats):
        top = acc[0, s]
        for f in range(1, dop_rows):
            top = jnp.maximum(top, acc[f, s])
        mine[s:s + 1, :] = jnp.max(top, axis=0, keepdims=True)
    for k in range(1, tm_count):
        share_peak(k).start()
    for f in range(dop_rows):
        for s in range(sats):
            power_ref[s, :, f, :] = acc[f, s]
    energy = jnp.zeros((8, inner), jnp.float32)
    for g in range(tm_count):
        x = everyone[g].astype(jnp.float32)
        energy = energy + jnp.sum((x * x).reshape(-1, 8, inner), axis=0)
    mean = jnp.sum(energy) * (sample_scale * sample_scale / float(blocks * sample_length))
    floor = jnp.maximum(mean, 0.25)
    for k in range(1, line):
        along_z(k).wait_send()
    if cores > 1:
        for k in range(line):
            to_twin(k).wait_send()
    for j in far:
        to_far(j).wait_send()
        for n, c in around:
            spread_far(j, n, c).wait_send()
    for k in near:
        whole_group(k, me_tm).wait_send()
    for k in range(1, tm_count):
        share_peak(k).wait()
    best = mine[...]
    for k in range(1, tm_count):
        best = jnp.maximum(best, peaks[k - 1])
    peak_ref[...] = best / floor


def stay(value):
    return pltpu.with_memory_space_constraint(value, pltpu.HBM)


def emit(power_ref, peak_ref, power_hbm, detection_hbm, detection, sems):
    copy = pltpu.make_async_copy(power_ref, power_hbm, sems.at[0])
    copy.start()
    best = jnp.max(peak_ref[...], axis=1, keepdims=True)
    shape = peak_ref.shape
    on = lax.broadcasted_iota(jnp.int32, shape, 0) == lax.broadcasted_iota(jnp.int32, shape, 1)
    row = jnp.sum(jnp.where(on, best, 0.0), axis=0)
    detection[...] = row[:detection.shape[0]]
    small = pltpu.make_async_copy(detection, detection_hbm, sems.at[1])
    small.start()
    copy.wait()
    small.wait()


def shards(samples, codes, dopplers):
    tm_count, sat_count = lax.axis_size("tm"), lax.axis_size("sat")
    own, segment = samples.shape[1], samples.shape[2]
    sample_length = segment * sat_count
    outer, rows = sample_length // LANES, segment // LANES
    sats, chip_count = codes.shape
    dop_rows = dopplers.shape[0] // tm_count
    cores = 2 if sat_count % 2 == 0 else 1
    line = sat_count // cores
    wide, narrow, starts = tables(sample_length, chip_count, rows)
    pad = (max(starts) // LANES + 2) * LANES
    pad = max(pad, -(-chip_count // LANES) * LANES)
    peak_rows = -(-sats // 8) * 8
    slots = max(dop_rows, 2)
    vm = pl.BlockSpec(memory_space=pltpu.VMEM)
    hbm = pl.BlockSpec(memory_space=pltpu.HBM)
    dma = pltpu.SemaphoreType.DMA
    packed = samples.reshape(2, own, rows, LANES).transpose(0, 2, 1, 3).reshape(2 * rows * own, LANES)
    power, peak = pl.pallas_call(
        functools.partial(kernel, starts, outer, chip_count, cores),
        out_shape=(
            jax.ShapeDtypeStruct((sats, outer, dop_rows, LANES), jnp.float32),
            jax.ShapeDtypeStruct((peak_rows, LANES), jnp.float32),
        ),
        in_specs=[hbm, hbm, hbm, hbm, hbm],
        out_specs=(vm, vm),
        scratch_shapes=[
            pltpu.VMEM(codes.shape, jnp.int32),
            pltpu.SMEM(dopplers.shape, jnp.int32),
            pltpu.VMEM(wide.shape, jnp.bfloat16),
            pltpu.VMEM(narrow.shape, jnp.float32),
            pltpu.VMEM((2, outer, 3 * outer), jnp.bfloat16),
            pltpu.VMEM((tm_count, cores, line, 2 * rows * own, LANES), jnp.int32),
            pltpu.VMEM((8, pad), jnp.float32),
            pltpu.VMEM((sats, outer, LANES), jnp.float32),
            pltpu.VMEM((sats, outer, 2 * LANES), jnp.float32),
            pltpu.VMEM((dop_rows, 2, outer, 3 * outer), jnp.bfloat16),
            pltpu.VMEM((dop_rows, 2, outer, LANES), jnp.float32),
            pltpu.VMEM((2, 2 * outer, own * LANES), jnp.bfloat16),
            pltpu.VMEM((slots, own * outer, 2 * LANES), jnp.float32),
            pltpu.VMEM((slots, sats, 2, 2 * outer, own * LANES), jnp.bfloat16),
            pltpu.VMEM((dop_rows, sats, outer, LANES), jnp.float32),
            pltpu.VMEM((tm_count - 1, peak_rows, LANES), jnp.float32),
            pltpu.VMEM((peak_rows, LANES), jnp.float32),
            dma((5,)),
            dma((line,)),
            dma((line,)),
            dma((line,)),
            dma((line,)),
            dma((sat_count,)),
            dma((sat_count,)),
            dma((tm_count - 1,)),
            dma((tm_count - 1,)),
            dma((tm_count - 1,)),
            dma((tm_count - 1,)),
        ],
        compiler_params=pltpu.CompilerParams(
            vmem_limit_bytes=KERNEL_BYTES, collective_id=0, has_side_effects=True),
        name="search",
    )(stay(packed), stay(codes), stay(dopplers), jnp.asarray(padded(wide, PADDING)), jnp.asarray(padded(narrow, PADDING)))
    power, detection = pl.pallas_call(
        emit,
        out_shape=(
            jax.ShapeDtypeStruct(power.shape, jnp.float32),
            jax.ShapeDtypeStruct((sats,), jnp.float32),
        ),
        in_specs=[vm, vm],
        out_specs=(hbm, hbm),
        scratch_shapes=[pltpu.VMEM((sats,), jnp.float32), dma((2,))],
        compiler_params=pltpu.CompilerParams(vmem_limit_bytes=2_000_000),
        name="emit",
    )(power, peak)
    power = power.transpose(2, 0, 1, 3).reshape(dop_rows, sats, sample_length)
    return power, detection


def solution(mesh):
    placed = (P(None, "tm", "sat"), P("sat", None), P())
    return jax.shard_map(
        shards,
        mesh=mesh,
        in_specs=placed,
        out_specs=(P("tm", "sat", None), P("sat")),
        check_vma=False,
    )
```

```python
import functools
import math

import jax
import jax.numpy as jnp
import ml_dtypes
import numpy as np
from jax import lax
from jax.experimental import pallas as pl
from jax.experimental.pallas import tpu as pltpu
from jax.sharding import PartitionSpec as P

sample_scale = 2.0 ** (-29)
wrap_count = 32768
LANES = 128
KERNEL_BYTES = 55_800_000
PADDING = 1_200_000
MESH = pl.DeviceIdType.MESH


def halves(table):
    high = table.astype(np.float32).astype(ml_dtypes.bfloat16)
    low = (table - high.astype(np.float64)).astype(np.float32).astype(ml_dtypes.bfloat16)
    return high, low


@functools.lru_cache(maxsize=None)
def tables(sample_length, chip_count, rows):
    inner = LANES
    outer = sample_length // inner
    a = np.arange(outer)
    c = np.arange(inner)
    ang_o = 2 * np.pi * (np.outer(a, a) % outer) / outer
    ang_t = 2 * np.pi * (np.outer(a, c) % sample_length) / sample_length
    ang_i = 2 * np.pi * (np.outer(c, c) % inner) / inner
    fc, fs = np.cos(ang_o), -np.sin(ang_o)
    first = np.block([[fc, -fs], [fs, fc]])
    second = np.block([[-fs, -fc], [fc, -fs]])
    wc, ws = np.cos(ang_i), -np.sin(ang_i)
    fh, fl = halves(np.block([[wc, ws], [-ws, wc]]))
    ih, il = halves(np.block([[wc, -ws], [ws, wc]]))
    full = np.block([[fc, fs], [-fs, fc]])
    half, span = outer // 2, rows // 2
    low = np.concatenate([np.arange(0, half, 2), np.arange(1, half, 2)])
    order = np.concatenate([low, low + half])
    both = np.concatenate([low, low + outer])
    spot = np.arange(outer)
    base = spot // rows * rows + spot % span * 2
    part = spot % rows // span
    column = np.concatenate([base, base + 1])
    picked = np.concatenate([part, part]) * outer + column
    first, second = first[both][:, picked], second[both][:, picked]
    keep = np.concatenate([np.arange(half), np.arange(half) + outer])
    backs = []
    for parity in range(2):
        side = np.arange(parity, outer, 2)
        bh, bl = halves(full[keep][:, np.concatenate([side, side + outer])])
        backs.append(np.concatenate([bh, bl], axis=1))
    ch, cl = halves(np.concatenate([fc[order], fs[order]], axis=0))
    offsets = np.arange(sample_length).reshape(outer, inner)
    chips = offsets * chip_count // sample_length
    signs = 1 - 2 * ((offsets * 2 * chip_count // sample_length) % 2)
    starts = tuple(int(v) for v in chips[:, 0])
    within = chips - chips[:, :1]
    wide = np.concatenate([fh, fh, fl, ih, ih, il], axis=0)
    ang_t = ang_t[order]
    narrow = [first, second, np.cos(ang_t), -np.sin(ang_t), *backs,
              np.concatenate([ch, cl], axis=1), within, signs, np.tile(column * inner, (8, 1))]
    narrow = np.concatenate([np.asarray(t, np.float32) for t in narrow], axis=0)
    return wide, narrow, starts


def padded(table, size):
    extra = -(-size // (table.shape[1] * table.dtype.itemsize)) - table.shape[0]
    return np.pad(table, ((0, max(extra, 0)), (0, 0)))


def split(value):
    high = value.astype(jnp.bfloat16)
    low = (value - high.astype(jnp.float32)).astype(jnp.bfloat16)
    return high, low


def rest(value):
    return value - value.astype(jnp.bfloat16).astype(jnp.float32)


def three(pieces, table):
    value = jnp.concatenate([jnp.concatenate(row, axis=1) for row in pieces], axis=0)
    low = jnp.concatenate([jnp.concatenate([rest(p) for p in row], axis=1) for row in pieces], axis=0)
    high, low = value.astype(jnp.bfloat16), low.astype(jnp.bfloat16)
    depth = high.shape[1]
    top, bottom = table[0:depth], table[2 * depth:3 * depth]
    count = high.shape[0]
    pair = mm(jnp.concatenate([high, low], axis=0), top)
    return pair[:count] + (pair[count:] + mm(high, bottom))


def mm(left, right):
    return jnp.dot(left, right, preferred_element_type=jnp.float32)


def flip(me, k, count):
    if count & (count - 1):
        return lax.rem(me + k, count)
    peer, bit = 0, 1
    while bit < count:
        peer = peer + ((me // bit + k // bit) % 2) * bit
        bit *= 2
    return peer


def back_flip(me, k, count):
    return lax.rem(me + count - k, count) if count & (count - 1) else flip(me, k, count)


def kernel(starts, outer, chip_count, cores, x_hbm, codes_hbm, dop_hbm, wide_hbm, narrow_hbm,
           power_ref, peak_ref, chips, dop_ref, wide, narrow, back,
           everyone, cpad, gath, cspec, rot, dtw, xs, spec, lagged, acc, peaks, mine,
           tab_sem, send_z, recv_z, send_twin, recv_twin, send_far, recv_far, send_tm, recv_tm,
           send_peak, recv_peak):
    inner = LANES
    tm_count, _, line, packed_rows, _ = everyone.shape
    dop_rows, sats = acc.shape[0], acc.shape[1]
    sample_length = outer * inner
    rows = outer // (cores * line)
    own = packed_rows // (2 * rows)
    half = outer // 2
    blocks = tm_count * own
    slots = spec.shape[0]
    me_tm, me_sat = lax.axis_index("tm"), lax.axis_index("sat")
    me_z, me_core = me_sat // cores, lax.rem(me_sat, cores)

    def place(z, core):
        return z * cores + core

    pairs = ((x_hbm, everyone.at[me_tm, me_core, me_z]), (codes_hbm, chips), (dop_hbm, dop_ref),
             (narrow_hbm.at[pl.ds(0, narrow.shape[0])], narrow),
             (wide_hbm.at[pl.ds(0, wide.shape[0])], wide))
    loads = [pltpu.make_async_copy(h, t, tab_sem.at[i]) for i, (h, t) in enumerate(pairs)]
    loads[0].start()

    around = [(k, c) for k in range(line) for c in range(cores) if k or c]
    far = [tm_count - 1] if tm_count > 2 else []
    near = [k for k in range(1, tm_count) if k not in far]
    barrier = pltpu.get_barrier_semaphore()
    for k, c in reversed(around):
        target = place(flip(me_z, k, line), flip(me_core, c, cores))
        pl.semaphore_signal(barrier, inc=1, device_id={"sat": target}, device_id_type=MESH)
    for k in range(1, tm_count):
        for c in range(cores):
            target = place(me_z, flip(me_core, c, cores))
            pl.semaphore_signal(
                barrier, inc=1, device_id={"tm": flip(me_tm, k, tm_count), "sat": target}, device_id_type=MESH)

    for load in loads[1:]:
        load.start()

    def pass_on(piece, sends, recvs, at, k, c):
        target = place(flip(me_z, k, line), flip(me_core, c, cores))
        return pltpu.make_async_remote_copy(
            src_ref=piece, dst_ref=piece, send_sem=sends.at[at], recv_sem=recvs.at[at],
            device_id={"sat": target}, device_id_type=MESH)

    def my_piece(z):
        return everyone.at[me_tm, me_core, z]

    def along_z(k):
        return pass_on(my_piece(me_z), send_z, recv_z, k, k, 0)

    def from_z(k):
        return pass_on(my_piece(back_flip(me_z, k, line)), send_z, recv_z, k, k, 0)

    def to_twin(k):
        return pass_on(my_piece(back_flip(me_z, k, line)), send_twin, recv_twin, k, 0, 1)

    def from_twin(k):
        piece = everyone.at[me_tm, back_flip(me_core, 1, cores), back_flip(me_z, k, line)]
        return pass_on(piece, send_twin, recv_twin, k, 0, 1)

    def far_group(k):
        return back_flip(me_tm, k, tm_count)

    def to_far(k):
        return pltpu.make_async_remote_copy(
            src_ref=my_piece(me_z), dst_ref=my_piece(me_z), send_sem=send_far.at[0], recv_sem=recv_far.at[0],
            device_id={"tm": flip(me_tm, k, tm_count)}, device_id_type=MESH)

    def from_far(k):
        piece = everyone.at[far_group(k), me_core, me_z]
        return pltpu.make_async_remote_copy(
            src_ref=piece, dst_ref=piece, send_sem=send_far.at[0], recv_sem=recv_far.at[0],
            device_id={"tm": flip(me_tm, k, tm_count)}, device_id_type=MESH)

    def spread_far(j, k, c):
        return pass_on(everyone.at[far_group(j), me_core, me_z], send_far, recv_far, k * cores + c, k, c)

    def gather_far(j, k, c):
        piece = everyone.at[far_group(j), back_flip(me_core, c, cores), back_flip(me_z, k, line)]
        return pass_on(piece, send_far, recv_far, k * cores + c, k, c)

    def relay(k, z):
        for c in range(cores):
            pltpu.make_async_remote_copy(
                src_ref=my_piece(z), dst_ref=my_piece(z), send_sem=send_tm.at[k - 1], recv_sem=recv_tm.at[k - 1],
                device_id={"tm": flip(me_tm, k, tm_count), "sat": place(me_z, flip(me_core, c, cores))},
                device_id_type=MESH).start()

    def whole_group(k, at):
        return pltpu.make_async_remote_copy(
            src_ref=everyone.at[at], dst_ref=everyone.at[at], send_sem=send_tm.at[k - 1],
            recv_sem=recv_tm.at[k - 1], device_id={"tm": flip(me_tm, k, tm_count)}, device_id_type=MESH)

    def share_peak(k):
        return pltpu.make_async_remote_copy(
            src_ref=mine, dst_ref=peaks.at[k - 1], send_sem=send_peak.at[k - 1],
            recv_sem=recv_peak.at[k - 1], device_id={"tm": flip(me_tm, k, tm_count)}, device_id_type=MESH)

    loads[0].wait()
    pl.semaphore_wait(barrier, len(around) + (tm_count - 1) * cores)
    for k in reversed(range(1, line)):
        along_z(k).start()
    for j in far:
        to_far(j).start()
    for j in near:
        relay(j, me_z)
    if cores > 1:
        to_twin(0).start()

    loads[1].wait()
    cpad[...] = jnp.zeros_like(cpad)
    cpad[0:sats, 0:chip_count] = chips[...].astype(jnp.float32)
    for n1 in range(outer):
        base = starts[n1] // LANES * LANES
        shift = starts[n1] - base
        piece = cpad[:, base:base + 2 * LANES]
        if shift:
            piece = pltpu.roll(piece, 2 * LANES - shift, 1)
        for s in range(sats):
            gath[s, n1:n1 + 1, :] = piece[s:s + 1, :LANES]
    for load in loads[2:]:
        load.wait()

    cut = [0]

    def take(count):
        cut.append(cut[-1] + count)
        return narrow[cut[-2]:cut[-1]]

    first, second = take(outer), take(outer)
    t_re, t_im = take(outer), take(outer)
    for parity in range(2):
        table = take(outer)
        bh, bl = table[:, :outer], table[:, outer:]
        back[parity] = jnp.concatenate([bh, bh, bl], axis=1).astype(jnp.bfloat16)
    code = take(2 * outer).astype(jnp.bfloat16)
    within = take(outer).astype(jnp.int32)
    signs = take(outer)
    row_of = take(8).astype(jnp.int32)
    t_at = 2 * outer
    fwd_ref = wide.at[pl.ds(0, 6 * inner)]
    inv_ref = wide.at[pl.ds(6 * inner, 6 * inner)]
    scale = math.sqrt(1.0 / (float(sample_length) ** 3 * blocks))
    for s in range(sats):
        rep = jnp.take_along_axis(gath[s], within, axis=1) * signs
        rep = rep.astype(jnp.bfloat16)
        y = mm(code, jnp.concatenate([rep, rep], axis=0))
        y_re, y_im = y[:outer], y[outer:]
        z = jnp.concatenate([y_re * t_re - y_im * t_im, y_re * t_im + y_im * t_re], axis=1)
        zh, zl = split(z)
        cspec[s] = mm(jnp.concatenate([zh, zl, zh], axis=1), fwd_ref[...]) * scale

    lane = lax.broadcasted_iota(jnp.int32, (8, inner), 1)
    base_row = me_tm * dop_rows
    turn = 2.0 * math.pi / wrap_count
    bins = lax.broadcasted_iota(jnp.int32, (8, inner), 0)
    for f0 in range(0, dop_rows, 4):
        d = jnp.zeros((8, inner), jnp.int32)
        for f in range(f0, min(f0 + 4, dop_rows)):
            d = jnp.where(lax.rem(bins, 4) == f - f0, dop_ref[base_row + f], d)
        m = (jnp.where(bins < 4, row_of, lane) * d) & (wrap_count - 1)
        angle = m.astype(jnp.float32) * turn
        cosine, sine = jnp.cos(angle), -jnp.sin(angle)
        for f in range(f0, min(f0 + 4, dop_rows)):
            i = f - f0
            c1, s1 = cosine[i:i + 1] * sample_scale, sine[i:i + 1] * sample_scale
            c2, s2 = cosine[i + 4:i + 5], sine[i + 4:i + 5]
            mix = first * c1 + second * s1
            low = mix - mix.astype(jnp.bfloat16).astype(jnp.float32)
            for parity in range(2):
                at = slice(parity * outer, (parity + 1) * outer)
                rot[f, parity] = jnp.concatenate([mix[:, at], mix[:, at], low[:, at]], axis=1).astype(jnp.bfloat16)
            dtw[f, 0] = t_re * c2 - t_im * s2
            dtw[f, 1] = t_re * s2 + t_im * c2
    acc[...] = jnp.zeros_like(acc)

    inside = ((me_z + 1) // 2) % 2 if line == 4 else 0
    for n in range(1, line):
        k = n
        if line == 4 and n > 1:
            k = 2 + inside if n == 2 else 3 - inside
        from_z(k).wait_recv()
        if cores > 1:
            to_twin(k).start()
        for j in near:
            relay(j, back_flip(me_z, k, line))
        if n == line // 2:
            for j in far:
                from_far(j).wait_recv()
                for i, c in around:
                    spread_far(j, i, c).start()
    if cores > 1:
        for k in range(line):
            from_twin(k).wait_recv()

    def arrive(j):
        g = back_flip(me_tm, j, tm_count)
        for parity in range(2):
            cols = []
            for blk in range(own):
                parts = [everyone[g, q % cores, q // cores, pl.ds(parity * own + blk, rows, stride=2 * own), :]
                         for q in range(cores * line)]
                cols.append(jnp.concatenate(parts, axis=0))
            xh, xl = split(jnp.concatenate(cols, axis=1).astype(jnp.float32))
            xs[parity, 0:outer] = xh
            xs[parity, outer:2 * outer] = xl

    def rotate(f):
        sides = []
        for parity in range(2):
            high, low = xs[parity, 0:outer], xs[parity, outer:2 * outer]
            sides.append(mm(rot[f, parity], jnp.concatenate([high, low, high], axis=0)))
        return sides

    def spectrum(f, sides):
        u_re, u_im = dtw[f, 0], dtw[f, 1]
        plus, minus = sides[0] + sides[1], sides[0] - sides[1]
        zs = []
        for blk in range(own):
            at = slice(blk * inner, (blk + 1) * inner)
            y_re = jnp.concatenate([plus[:half, at], minus[:half, at]], axis=0)
            y_im = jnp.concatenate([plus[half:, at], minus[half:, at]], axis=0)
            zs.append((y_re * u_re - y_im * u_im, y_re * u_im + y_im * u_re))
        spec[f % slots] = three(zs, fwd_ref)

    def cross(f, s):
        crosses = []
        k_re, k_im = cspec[s, :, :inner], cspec[s, :, inner:]
        for blk in range(own):
            s_re = spec[f % slots, blk * outer:(blk + 1) * outer, :inner]
            s_im = spec[f % slots, blk * outer:(blk + 1) * outer, inner:]
            crosses.append((s_re * k_re + s_im * k_im, s_im * k_re - s_re * k_im))
        lag = three(crosses, inv_ref)
        w_re, w_im = narrow[t_at:t_at + outer], narrow[t_at + outer:t_at + 2 * outer]
        quarter = outer // 4
        cols = ([], [])
        for blk in range(own):
            at = blk * outer
            l_re, l_im = lag[at:at + outer, :inner], lag[at:at + outer, inner:]
            v_re, v_im = l_re * w_re + l_im * w_im, l_im * w_re - l_re * w_im
            for parity in range(2):
                one = slice(parity * quarter, (parity + 1) * quarter)
                two = slice(half + parity * quarter, half + (parity + 1) * quarter)
                cols[parity].append(jnp.concatenate([v_re[one], v_re[two], v_im[one], v_im[two]], axis=0))
        for parity in range(2):
            wh, wl = split(jnp.concatenate(cols[parity], axis=1))
            lagged[f % slots, s, parity, 0:outer] = wh
            lagged[f % slots, s, parity, outer:2 * outer] = wl

    def finish(f, s):
        sides = []
        for parity in range(2):
            high, low = lagged[f % slots, s, parity, 0:outer], lagged[f % slots, s, parity, outer:2 * outer]
            sides.append(mm(back[parity], jnp.concatenate([high, low, high], axis=0)))
        for at, out in ((0, sides[0] + sides[1]), (half, sides[0] - sides[1])):
            o_re, o_im = out[:half], out[half:]
            p = o_re * o_re + o_im * o_im
            total = p[:, :inner]
            for blk in range(1, own):
                total = total + p[:, blk * inner:(blk + 1) * inner]
            acc[f, s, at:at + half] += total

    def step(f, forward, middle, last):
        if forward:
            y = rotate(f)
        for s in range(sats):
            if middle:
                cross((f - 1) % dop_rows, s)
            if s == max(sats - 2, 0) and forward:
                spectrum(f, y)
            if last:
                finish((f - 2) % dop_rows, s)

    def group(j, first=False):
        for f in range(dop_rows):
            if f == 0:
                arrive(j)
            step(f, True, not first or f >= 1, not first or f >= 2)

    def await_near(j):
        whole_group(j, back_flip(me_tm, j, tm_count)).wait_recv()

    def near_group(j, carry):
        await_near(j)
        group(j)
        return carry

    group(0, True)
    if len(near) <= 3:
        for j in near:
            await_near(j)
        for j in near:
            group(j)
    else:
        lax.fori_loop(1, len(near) + 1, near_group, 0)
    for j in far:
        for n, c in around:
            gather_far(j, n, c).wait_recv()
        group(j)
    for f in range(2):
        step(f, False, f == 0, True)

    mine[...] = jnp.zeros_like(mine)
    for s in range(sats):
        top = acc[0, s]
        for f in range(1, dop_rows):
            top = jnp.maximum(top, acc[f, s])
        mine[s:s + 1, :] = jnp.max(top, axis=0, keepdims=True)
    for k in range(1, tm_count):
        share_peak(k).start()
    for f in range(dop_rows):
        for s in range(sats):
            power_ref[s, :, f, :] = acc[f, s]
    energy = jnp.zeros((8, inner), jnp.float32)
    for g in range(tm_count):
        x = everyone[g].astype(jnp.float32)
        energy = energy + jnp.sum((x * x).reshape(-1, 8, inner), axis=0)
    mean = jnp.sum(energy) * (sample_scale * sample_scale / float(blocks * sample_length))
    floor = jnp.maximum(mean, 0.25)
    for k in range(1, line):
        along_z(k).wait_send()
    if cores > 1:
        for k in range(line):
            to_twin(k).wait_send()
    for j in far:
        to_far(j).wait_send()
        for n, c in around:
            spread_far(j, n, c).wait_send()
    for k in near:
        whole_group(k, me_tm).wait_send()
    for k in range(1, tm_count):
        share_peak(k).wait()
    best = mine[...]
    for k in range(1, tm_count):
        best = jnp.maximum(best, peaks[k - 1])
    peak_ref[...] = best / floor


def stay(value):
    return pltpu.with_memory_space_constraint(value, pltpu.HBM)


def emit(power_ref, peak_ref, power_hbm, detection_hbm, detection, sems):
    copy = pltpu.make_async_copy(power_ref, power_hbm, sems.at[0])
    copy.start()
    best = jnp.max(peak_ref[...], axis=1, keepdims=True)
    shape = peak_ref.shape
    on = lax.broadcasted_iota(jnp.int32, shape, 0) == lax.broadcasted_iota(jnp.int32, shape, 1)
    row = jnp.sum(jnp.where(on, best, 0.0), axis=0)
    detection[...] = row[:detection.shape[0]]
    small = pltpu.make_async_copy(detection, detection_hbm, sems.at[1])
    small.start()
    copy.wait()
    small.wait()


def shards(samples, codes, dopplers):
    tm_count, sat_count = lax.axis_size("tm"), lax.axis_size("sat")
    own, segment = samples.shape[1], samples.shape[2]
    sample_length = segment * sat_count
    outer, rows = sample_length // LANES, segment // LANES
    sats, chip_count = codes.shape
    dop_rows = dopplers.shape[0] // tm_count
    cores = 2 if sat_count % 2 == 0 else 1
    line = sat_count // cores
    wide, narrow, starts = tables(sample_length, chip_count, rows)
    pad = (max(starts) // LANES + 2) * LANES
    pad = max(pad, -(-chip_count // LANES) * LANES)
    peak_rows = -(-sats // 8) * 8
    slots = max(dop_rows, 2)
    vm = pl.BlockSpec(memory_space=pltpu.VMEM)
    hbm = pl.BlockSpec(memory_space=pltpu.HBM)
    dma = pltpu.SemaphoreType.DMA
    packed = samples.reshape(2, own, rows, LANES).transpose(0, 2, 1, 3).reshape(2 * rows * own, LANES)
    power, peak = pl.pallas_call(
        functools.partial(kernel, starts, outer, chip_count, cores),
        out_shape=(
            jax.ShapeDtypeStruct((sats, outer, dop_rows, LANES), jnp.float32),
            jax.ShapeDtypeStruct((peak_rows, LANES), jnp.float32),
        ),
        in_specs=[hbm, hbm, hbm, hbm, hbm],
        out_specs=(vm, vm),
        scratch_shapes=[
            pltpu.VMEM(codes.shape, jnp.int32),
            pltpu.SMEM(dopplers.shape, jnp.int32),
            pltpu.VMEM(wide.shape, jnp.bfloat16),
            pltpu.VMEM(narrow.shape, jnp.float32),
            pltpu.VMEM((2, outer, 3 * outer), jnp.bfloat16),
            pltpu.VMEM((tm_count, cores, line, 2 * rows * own, LANES), jnp.int32),
            pltpu.VMEM((8, pad), jnp.float32),
            pltpu.VMEM((sats, outer, LANES), jnp.float32),
            pltpu.VMEM((sats, outer, 2 * LANES), jnp.float32),
            pltpu.VMEM((dop_rows, 2, outer, 3 * outer), jnp.bfloat16),
            pltpu.VMEM((dop_rows, 2, outer, LANES), jnp.float32),
            pltpu.VMEM((2, 2 * outer, own * LANES), jnp.bfloat16),
            pltpu.VMEM((slots, own * outer, 2 * LANES), jnp.float32),
            pltpu.VMEM((slots, sats, 2, 2 * outer, own * LANES), jnp.bfloat16),
            pltpu.VMEM((dop_rows, sats, outer, LANES), jnp.float32),
            pltpu.VMEM((tm_count - 1, peak_rows, LANES), jnp.float32),
            pltpu.VMEM((peak_rows, LANES), jnp.float32),
            dma((5,)),
            dma((line,)),
            dma((line,)),
            dma((line,)),
            dma((line,)),
            dma((sat_count,)),
            dma((sat_count,)),
            dma((tm_count - 1,)),
            dma((tm_count - 1,)),
            dma((tm_count - 1,)),
            dma((tm_count - 1,)),
        ],
        compiler_params=pltpu.CompilerParams(
            vmem_limit_bytes=KERNEL_BYTES, collective_id=0, has_side_effects=True),
        name="search",
    )(stay(packed), stay(codes), stay(dopplers), jnp.asarray(padded(wide, PADDING)), jnp.asarray(padded(narrow, PADDING)))
    power, detection = pl.pallas_call(
        emit,
        out_shape=(
            jax.ShapeDtypeStruct(power.shape, jnp.float32),
            jax.ShapeDtypeStruct((sats,), jnp.float32),
        ),
        in_specs=[vm, vm],
        out_specs=(hbm, hbm),
        scratch_shapes=[pltpu.VMEM((sats,), jnp.float32), dma((2,))],
        compiler_params=pltpu.CompilerParams(vmem_limit_bytes=2_000_000),
        name="emit",
    )(power, peak)
    power = power.transpose(2, 0, 1, 3).reshape(dop_rows, sats, sample_length)
    return power, detection


def solution(mesh):
    placed = (P(None, "tm", "sat"), P("sat", None), P())
    return jax.shard_map(
        shards,
        mesh=mesh,
        in_specs=placed,
        out_specs=(P("tm", "sat", None), P("sat")),
        check_vma=False,
    )
```
